8 devices in a mesh: dp: 1 (over z), cp: 2 (over y), tp: 4 (over x, core).
Axes of the slice: x: 2, y: 2, z: 1, core: 2. Of those that a mesh axis runs over, the one named last changes fastest.
Arguments:
- x: bfloat16 [3072, 3584], P(('dp', 'cp', 'tp'))
- idx: int32 [3072, 2], P(('dp', 'cp', 'tp'))
- gates: float32 [3072, 2], P(('dp', 'cp', 'tp'))
- wq: bfloat16 [3584, 3584], P(None, 'tp')
- wk: bfloat16 [3584, 512], P(None, 'tp')
- wv: bfloat16 [3584, 512], P(None, 'tp')
- wo: bfloat16 [3584, 3584], P('tp')
- w1g: bfloat16 [8, 3584, 2560], P(('cp', 'tp'))
- w1u: bfloat16 [8, 3584, 2560], P(('cp', 'tp'))
- w2: bfloat16 [8, 2560, 3584], P(('cp', 'tp'))
Outputs:
- output: bfloat16 [3072, 3584], P(('dp', 'cp', 'tp'))
All inputs are finite; a program needn't handle non-finite values.
Results may differ from the reference program's by a relative error of at most 0.00918231.
Values are sent between devices in bfloat16 or wider.
A program may use at most 1 GiB of HBM per device.

```python
import math
import jax
import jax.numpy as jnp
from jax import lax

H = 3584
FF = 2560
HEADS = 28
KV_HEADS = 4
HEAD = 128
S = 3072
CP = 2
TP = 4
TOP = 2
QBLK = 512

E = CP * TP
T = S // E
CAP = 4 * T // E
M = 2 * T // E


def seg_positions():
    i = jnp.arange(S, dtype=jnp.int32)
    seg = S // (2 * CP)
    b = i // seg
    r = b // 2
    s_id = jnp.where(b % 2 == 0, r, 2 * CP - 1 - r)
    return s_id * seg + i % seg


def source_routing(key, sigma, counts):
    ends = jnp.cumsum(counts)
    labels = sigma[jnp.searchsorted(ends, jnp.arange(2 * T, dtype=jnp.int32), side='right')]
    perm = jax.random.permutation(key, T)
    return jnp.stack([labels[perm], labels[perm + T]], axis=1).astype(jnp.int32)


def setup_inputs(seed: int = 0, part: int = 0) -> dict:
    key = jax.random.key(seed)
    ks = jax.random.split(key, 7)
    kx = jax.random.split(jax.random.fold_in(key, part), 4)
    a = math.log(S / 16.0) ** 0.25

    def nrm(k, shape, scale):
        return (jax.random.normal(k, shape, jnp.float32) * scale).astype(jnp.bfloat16)

    wq = nrm(ks[0], (H, HEADS * HEAD), a / math.sqrt(H))
    wk = nrm(ks[1], (H, KV_HEADS * HEAD), a / math.sqrt(H))
    wv = nrm(ks[2], (H, KV_HEADS * HEAD), 1.0 / math.sqrt(H))
    wo = nrm(ks[3], (HEADS * HEAD, H), 1.0 / math.sqrt(HEADS * HEAD))
    w1g = nrm(ks[4], (E, H, FF), 1.0 / math.sqrt(H))
    w1u = nrm(ks[5], (E, H, FF), 1.0 / math.sqrt(H))
    w2 = nrm(ks[6], (E, FF, H), 1.5 / math.sqrt(FF))
    x = nrm(kx[0], (S, H), 1.0)
    sigmas = jax.vmap(lambda kk: jax.random.permutation(kk, E))(jax.random.split(kx[1], E))
    counts = jnp.full((E,), M, jnp.int32)
    idx = jax.vmap(lambda kk, sg: source_routing(kk, sg, counts))(jax.random.split(kx[2], E), sigmas)
    idx = idx.reshape(S, TOP)
    gates = jax.random.uniform(kx[3], (S, TOP), jnp.float32, 0.3, 0.7)
    return {'x': x, 'idx': idx, 'gates': gates, 'wq': wq, 'wk': wk, 'wv': wv, 'wo': wo, 'w1g': w1g, 'w1u': w1u, 'w2': w2}


def reference(x, idx, gates, wq, wk, wv, wo, w1g, w1u, w2):
    pos = seg_positions()
    g = HEADS // KV_HEADS
    q = jnp.dot(x, wq, preferred_element_type=jnp.float32).astype(jnp.bfloat16)
    k = jnp.dot(x, wk, preferred_element_type=jnp.float32).astype(jnp.bfloat16)
    v = jnp.dot(x, wv, preferred_element_type=jnp.float32).astype(jnp.bfloat16)
    qh = q.reshape(S, HEADS, HEAD).transpose(1, 0, 2)
    kh = jnp.repeat(k.reshape(S, KV_HEADS, HEAD).transpose(1, 0, 2), g, axis=0)
    vh = jnp.repeat(v.reshape(S, KV_HEADS, HEAD).transpose(1, 0, 2), g, axis=0)
    scale = HEAD ** -0.5
    nb = S // QBLK

    def head(args):
        qa, ka, va = args

        def block(bargs):
            qb, pb = bargs
            s = jnp.dot(qb, ka.T, preferred_element_type=jnp.float32) * scale
            mask = pos[None, :] <= pb[:, None]
            s = jnp.where(mask, s, -1e30)
            m = jnp.max(s, axis=-1, keepdims=True)
            w = jnp.where(mask, jnp.exp(s - m), 0.0)
            l = jnp.sum(w, axis=-1, keepdims=True)
            ob = jnp.dot(w.astype(jnp.bfloat16), va, preferred_element_type=jnp.float32)
            return ob / l

        out = lax.map(block, (qa.reshape(nb, QBLK, HEAD), pos.reshape(nb, QBLK)))
        return out.reshape(S, HEAD)

    o = lax.map(head, (qh, kh, vh))
    o = o.transpose(1, 0, 2).reshape(S, HEADS * HEAD).astype(jnp.bfloat16)
    att = jnp.dot(o, wo, preferred_element_type=jnp.float32)
    h = (x.astype(jnp.float32) + att).astype(jnp.bfloat16)

    ea = idx.reshape(-1)
    tok = jnp.arange(S * TOP) // TOP
    onehot = (ea[:, None] == jnp.arange(E)[None, :]).astype(jnp.int32)
    slot = jnp.take_along_axis(jnp.cumsum(onehot, axis=0), ea[:, None], axis=1)[:, 0] - 1
    ct = E * CAP
    buf = jnp.zeros((E, ct, H), jnp.bfloat16).at[ea, slot].set(h[tok])

    def expert(args):
        rows, wg, wu, wd = args
        gg = jnp.dot(rows, wg, preferred_element_type=jnp.float32)
        uu = jnp.dot(rows, wu, preferred_element_type=jnp.float32)
        act = (jax.nn.silu(gg) * uu).astype(jnp.bfloat16)
        return jnp.dot(act, wd, preferred_element_type=jnp.float32).astype(jnp.bfloat16)

    z = lax.map(expert, (buf, w1g, w1u, w2))
    zt = z[ea, slot].astype(jnp.float32).reshape(S, TOP, H)
    y = h.astype(jnp.float32) + jnp.sum(gates[:, :, None] * zt, axis=1)
    return y.astype(jnp.bfloat16)
```

```python
import functools
import math
import jax, jax.numpy as jnp
from jax import lax
from jax.experimental import pallas as pl
from jax.experimental.pallas import tpu as pltpu
from jax.sharding import PartitionSpec as P
D=128
def attn_kernel(seg, bq, bk, heads, cp, q_ref, kv_ref, o_ref, m_ref, l_ref, acc_ref):
    rank = lax.axis_index('cp')
    i = pl.program_id(0)
    per = seg // bq
    s_id = jnp.where(i < per, rank, 2*cp-1-rank)
    nfull = s_id*per + lax.rem(i, per)
    c = D**-0.5*math.log2(math.e)
    def scores(h, j):
        k = kv_ref[pl.ds(pl.multiple_of(j*bk, bk), bk), :D]
        q = q_ref[:, h*D:(h+1)*D]
        return lax.dot_general(q, k, (((1,),(1,)),((),())), preferred_element_type=jnp.float32)
    def pv(p, j):
        v = kv_ref[pl.ds(pl.multiple_of(j*bk, bk), bk), D:]
        return jnp.dot(p.astype(jnp.bfloat16), v, preferred_element_type=jnp.float32)
    def lanes(p):
        t = p[:, :128]
        for a in range(128, bk, 128):
            t = t + p[:, a:a+128]
        return t
    mask = lax.broadcasted_iota(jnp.int32,(bq,bk),1) <= lax.broadcasted_iota(jnp.int32,(bq,bk),0)
    for h in range(heads):
        s = jnp.where(mask, scores(h, nfull)*c, -1e30)
        m = jnp.max(s, axis=1, keepdims=True)
        p = jnp.where(mask, jnp.exp2(s-m), 0.0)
        m_ref[h] = jnp.broadcast_to(m,(bq,128))
        l_ref[h] = lanes(p)
        acc_ref[h] = pv(p, nfull)
    def body(j, _):
        for h in range(heads):
            s = scores(h, j)*c
            mo = m_ref[h]
            mn = jnp.maximum(mo, jnp.max(s, axis=1, keepdims=True))
            p = jnp.exp2(s - jnp.concatenate([mn]*(bk//128),axis=1))
            al = jnp.exp2(mo-mn)
            m_ref[h] = mn
            l_ref[h] = l_ref[h]*al + lanes(p)
            acc_ref[h] = acc_ref[h]*al + pv(p, j)
        return 0
    lax.fori_loop(0, nfull, body, 0)
    for h in range(heads):
        l = jnp.sum(l_ref[h], axis=1, keepdims=True)
        o_ref[:, h*D:(h+1)*D] = (acc_ref[h]/l).astype(jnp.bfloat16)

def attention(q, kv, cp, bq=256, bk=256):
    n, hd = q.shape
    heads = hd//D
    seg = n//2
    return pl.pallas_call(
        functools.partial(attn_kernel, seg, bq, bk, heads, cp),
        grid=(n//bq,),
        in_specs=[pl.BlockSpec((bq,hd), lambda i:(i,0)), pl.BlockSpec(kv.shape, lambda i:(0,0))],
        out_specs=pl.BlockSpec((bq,hd), lambda i:(i,0)),
        out_shape=jax.ShapeDtypeStruct((n,hd), jnp.bfloat16),
        scratch_shapes=[pltpu.VMEM((heads,bq,128),jnp.float32)]*3,
        compiler_params=pltpu.CompilerParams(vmem_limit_bytes=60*1024*1024),
        name='attn')(q, kv)


def expert_ffn(rows, wg, wu, wd):
    gg = jnp.dot(rows, wg, preferred_element_type=jnp.float32)
    uu = jnp.dot(rows, wu, preferred_element_type=jnp.float32)
    act = (jax.nn.silu(gg) * uu).astype(jnp.bfloat16)
    return jnp.dot(act, wd, preferred_element_type=jnp.float32).astype(jnp.bfloat16)


def attention_residual(x, wq, wk, wv, wo, cp):
    xs = lax.all_gather(x, 'tp', axis=0, tiled=True)
    seg = xs.shape[0] // 2
    wkv = jnp.concatenate([wk, wv], axis=1)
    kv = jnp.dot(xs, wkv, preferred_element_type=jnp.float32).astype(jnp.bfloat16)
    kvs = lax.all_gather(kv, 'cp', axis=0)
    q = jnp.dot(xs, wq, preferred_element_type=jnp.float32).astype(jnp.bfloat16)
    kvp = jnp.concatenate([kvs[r, :seg] for r in range(cp)] + [kvs[r, seg:] for r in reversed(range(cp))], axis=0)
    o = attention(q, kvp, cp)
    part = jnp.dot(o, wo, preferred_element_type=jnp.float32)
    att = lax.psum_scatter(part, 'tp', scatter_dimension=0, tiled=True)
    return (x.astype(jnp.float32) + att).astype(jnp.bfloat16)


def routing(idx, ne):
    t = idx.shape[0]
    it = idx.T
    hit = (it[0][None, :] == jnp.arange(ne)[:, None]) | (it[1][None, :] == jnp.arange(ne)[:, None])
    before = (jnp.arange(t)[:, None] < jnp.arange(t)[None, :]).astype(jnp.bfloat16)
    rank = jnp.dot(hit.astype(jnp.bfloat16), before, preferred_element_type=jnp.float32).astype(jnp.int32)
    return jnp.where(hit, rank, -1)


def solution(mesh):
    cp = mesh.shape['cp']
    tp = mesh.shape['tp']
    ne = cp * tp
    rows_spec = P(('dp', 'cp', 'tp'), None)
    exp_spec = P(('cp', 'tp'), None, None)

    def local(x, idx, gates, wq, wk, wv, wo, w1g, w1u, w2):
        t, hd = x.shape
        cap = 4 * t // ne
        slot = routing(idx, ne)
        h = attention_residual(x, wq, wk, wv, wo, cp)
        pick = (slot[:, None, :] == jnp.arange(cap)[None, :, None]).astype(jnp.bfloat16).reshape(ne * cap, t)
        send = jnp.dot(pick, h, preferred_element_type=jnp.float32).astype(jnp.bfloat16)
        recv = lax.all_to_all(send.reshape(ne, cap, hd), ('cp', 'tp'), 0, 0, tiled=True)
        z = expert_ffn(recv.reshape(ne * cap, hd), w1g[0], w1u[0], w2[0])
        back = lax.all_to_all(z.reshape(ne, cap, hd), ('cp', 'tp'), 0, 0, tiled=True).reshape(ne * cap, hd)
        flat = jnp.arange(ne * cap)
        y = h.astype(jnp.float32)
        for k in range(2):
            mine = jnp.sum(jnp.where(idx[:, k][None, :] == jnp.arange(ne)[:, None], jnp.arange(ne)[:, None] * cap + slot, 0), axis=0)
            sel = (mine[:, None] == flat[None, :]).astype(jnp.bfloat16)
            y = y + gates[:, k:k + 1] * jnp.dot(sel, back, preferred_element_type=jnp.float32)
        return y.astype(jnp.bfloat16)

    return jax.shard_map(local, mesh=mesh, in_specs=(rows_spec, rows_spec, rows_spec, P(None, 'tp'), P(None, 'tp'), P(None, 'tp'), P('tp', None), exp_spec, exp_spec, exp_spec), out_specs=rows_spec, check_vma=False)
```

```python
import functools
import math

import jax
import jax.numpy as jnp
from jax import lax
from jax.experimental import pallas as pl
from jax.experimental.pallas import tpu as pltpu
from jax.sharding import PartitionSpec as P

D=128
def attn_kernel(seg, bq, bk, heads, cp, q_ref, kv_ref, o_ref, m_ref, l_ref, acc_ref):
    rank = lax.axis_index('cp')
    i = pl.program_id(0)
    per = seg // bq
    s_id = jnp.where(i < per, rank, 2*cp-1-rank)
    nfull = s_id*per + lax.rem(i, per)
    c = D**-0.5*math.log2(math.e)
    def scores(h, j):
        k = kv_ref[pl.ds(pl.multiple_of(j*bk, bk), bk), :D]
        q = q_ref[:, h*D:(h+1)*D]
        return lax.dot_general(q, k, (((1,),(1,)),((),())), preferred_element_type=jnp.float32)
    def pv(p, j):
        v = kv_ref[pl.ds(pl.multiple_of(j*bk, bk), bk), D:]
        return jnp.dot(p.astype(jnp.bfloat16), v, preferred_element_type=jnp.float32)
    def lanes(p):
        t = p[:, :128]
        for a in range(128, bk, 128):
            t = t + p[:, a:a+128]
        return t
    mask = lax.broadcasted_iota(jnp.int32,(bq,bk),1) <= lax.broadcasted_iota(jnp.int32,(bq,bk),0)
    for h in range(heads):
        s = jnp.where(mask, scores(h, nfull)*c, -1e30)
        m = jnp.max(s, axis=1, keepdims=True)
        p = jnp.where(mask, jnp.exp2(s-m), 0.0)
        m_ref[h] = jnp.broadcast_to(m,(bq,128))
        l_ref[h] = lanes(p)
        acc_ref[h] = pv(p, nfull)
    def body(j, _):
        for h in range(heads):
            s = scores(h, j)*c
            mo = m_ref[h]
            mn = jnp.maximum(mo, jnp.max(s, axis=1, keepdims=True))
            p = jnp.exp2(s - jnp.concatenate([mn]*(bk//128),axis=1))
            al = jnp.exp2(mo-mn)
            m_ref[h] = mn
            l_ref[h] = l_ref[h]*al + lanes(p)
            acc_ref[h] = acc_ref[h]*al + pv(p, j)
        return 0
    lax.fori_loop(0, nfull, body, 0)
    for h in range(heads):
        l = jnp.sum(l_ref[h], axis=1, keepdims=True)
        o_ref[:, h*D:(h+1)*D] = (acc_ref[h]/l).astype(jnp.bfloat16)

def attention(q, kv, cp, bq=256, bk=256):
    n, hd = q.shape
    heads = hd//D
    seg = n//2
    return pl.pallas_call(
        functools.partial(attn_kernel, seg, bq, bk, heads, cp),
        grid=(n//bq,),
        in_specs=[pl.BlockSpec((bq,hd), lambda i:(i,0)), pl.BlockSpec(kv.shape, lambda i:(0,0))],
        out_specs=pl.BlockSpec((bq,hd), lambda i:(i,0)),
        out_shape=jax.ShapeDtypeStruct((n,hd), jnp.bfloat16),
        scratch_shapes=[pltpu.VMEM((heads,bq,128),jnp.float32)]*3,
        compiler_params=pltpu.CompilerParams(vmem_limit_bytes=60*1024*1024),
        name='attn')(q, kv)


MESH = pl.DeviceIdType.MESH
NEAR = 6
FT = 256
NT = 512


def peer(r):
    c, t = lax.axis_index('cp'), lax.axis_index('tp')
    core, xx = lax.rem(t, 2), t // 2
    core = 1 - core if r & 1 else core
    xx = 1 - xx if r & 2 else xx
    c = 1 - c if r & 4 else c
    return c, xx * 2 + core


def device(r):
    c, t = peer(r)
    return (lax.axis_index('dp'), c, t)


def greet(peers):
    bar = pltpu.get_barrier_semaphore()
    for r in peers:
        pl.semaphore_signal(bar, inc=1, device_id=device(r), device_id_type=MESH)
    pl.semaphore_wait(bar, len(peers))


def moe_kernel(ne, cap, h_ref, slot_ref, flat_ref, gate_ref, w1g_ref, w1u_ref, w2_ref, y_ref,
               send, recv, act, zsend, zrecv, pick, w1b, w2b, ds, dr, zs, zr, w1s, w2s):
    t, hd = h_ref.shape
    ff = w2_ref.shape[0]
    nf, nz = ff // FT, hd // NT

    def w1_copy(tile, slot, which):
        src = (w1g_ref, w1u_ref)[which]
        return pltpu.make_async_copy(src.at[:, pl.ds(pl.multiple_of(tile * FT, FT), FT)], w1b.at[slot, which], w1s.at[slot, which])

    def w2_copy(tile, slot):
        return pltpu.make_async_copy(w2_ref.at[:, pl.ds(pl.multiple_of(tile * NT, NT), NT)], w2b.at[slot], w2s.at[slot])

    for s in range(2):
        w1_copy(s, s, 0).start()
        w1_copy(s, s, 1).start()
    for s in range(2):
        w2_copy(s, s).start()

    def out_copy(r):
        return pltpu.make_async_remote_copy(src_ref=send.at[r], dst_ref=recv.at[r], send_sem=ds.at[r], recv_sem=dr.at[r], device_id=device(r), device_id_type=MESH)

    def dispatch(r, dst):
        c, tt = peer(r)
        row = slot_ref[pl.ds(c * (ne // 2) + tt, 1), :]
        sel = (jnp.broadcast_to(row, (cap, t)) == lax.broadcasted_iota(jnp.int32, (cap, t), 0)).astype(jnp.bfloat16)

        def tile(n, _):
            cols = pl.ds(pl.multiple_of(n * NT, NT), NT)
            dst[r, :, cols] = jnp.dot(sel, h_ref[:, cols], preferred_element_type=jnp.float32).astype(jnp.bfloat16)
            return 0
        lax.fori_loop(0, nz, tile, 0)

    order = (2, 4, 3, 5, 6, 7, 1)
    dispatch(order[0], send)
    greet(range(1, ne))
    for a, r in enumerate(order):
        if a + 1 < len(order):
            dispatch(order[a + 1], send)
        else:
            dispatch(0, recv)
        out_copy(r).start()
    for k in range(2):
        pick[k * t:(k + 1) * t, :] = (flat_ref[:, k:k + 1] == lax.broadcasted_iota(jnp.int32, (t, ne * cap), 1)).astype(jnp.bfloat16)

    def back_copy(r, tile):
        cols = pl.ds(pl.multiple_of(tile * NT, NT), NT)
        return pltpu.make_async_remote_copy(src_ref=zsend.at[r, :, cols], dst_ref=zrecv.at[r, :, cols], send_sem=zs.at[r], recv_sem=zr.at[r], device_id=device(r), device_id_type=MESH)

    def experts(lo, hi, again):
        rows = (hi - lo) * cap
        off = 0 if again else nz

        def up(f, _):
            slot = lax.rem(f, 2)
            w1_copy(f, slot, 0).wait()
            w1_copy(f, slot, 1).wait()
            xr = recv[lo:hi].reshape(rows, hd)
            gg = jnp.dot(xr, w1b[slot, 0], preferred_element_type=jnp.float32)
            uu = jnp.dot(xr, w1b[slot, 1], preferred_element_type=jnp.float32)
            act[:rows, pl.ds(pl.multiple_of(f * FT, FT), FT)] = (gg * jax.nn.sigmoid(gg) * uu).astype(jnp.bfloat16)
            nxt = f + 2

            @pl.when(nxt < (nf + 2 if again else nf))
            def _():
                w1_copy(lax.rem(nxt, nf), slot, 0).start()
                w1_copy(lax.rem(nxt, nf), slot, 1).start()
            return 0
        lax.fori_loop(0, nf, up, 0)

        def down(n, _):
            slot = lax.rem(n + off, 2)
            w2_copy(n, slot).wait()

            @pl.when(n > 0)
            def _():
                for r in range(max(lo, 1), hi):
                    back_copy(r, n - 1).start()
            zz = jnp.dot(act[:rows], w2b[slot], preferred_element_type=jnp.float32).astype(jnp.bfloat16)
            cols = pl.ds(pl.multiple_of(n * NT, NT), NT)
            for r in range(lo, hi):
                dst = zrecv if r == 0 else zsend
                dst[r, :, cols] = zz[(r - lo) * cap:(r - lo + 1) * cap]
            nxt = n + 2

            @pl.when(nxt < (nz + 2 if again else nz))
            def _():
                w2_copy(lax.rem(nxt, nz), slot).start()
            return 0
        lax.fori_loop(0, nz, down, 0)
        for r in range(max(lo, 1), hi):
            back_copy(r, nz - 1).start()

    for r in range(1, NEAR):
        out_copy(r).wait_recv()
    experts(0, NEAR, True)
    for r in range(NEAR, ne):
        out_copy(r).wait_recv()
    experts(NEAR, ne, False)
    whole = lambda r: pltpu.make_async_remote_copy(src_ref=zsend.at[r], dst_ref=zrecv.at[r], send_sem=zs.at[r], recv_sem=zr.at[r], device_id=device(r), device_id_type=MESH)
    for r in range(1, ne):
        whole(r).wait_recv()

    def combine(n, _):
        cols = pl.ds(pl.multiple_of(n * NT, NT), NT)
        zt = jnp.dot(pick[...], zrecv[:, :, cols].reshape(ne * cap, NT), preferred_element_type=jnp.float32)
        y = h_ref[:, cols].astype(jnp.float32) + (gate_ref[:, 0:1] * zt[:t] + gate_ref[:, 1:2] * zt[t:])
        y_ref[:, cols] = y.astype(jnp.bfloat16)
        return 0
    lax.fori_loop(0, nz, combine, 0)
    for r in range(1, ne):
        out_copy(r).wait_send()
        whole(r).wait_send()


def moe_fast(h, slot, idx, gates, w1g, w1u, w2, cap, cid):
    t, hd = h.shape
    ne = slot.shape[0]
    me = lax.axis_index('cp') * (ne // 2) + lax.axis_index('tp')
    e = jnp.arange(ne)
    flat = []
    for k in range(2):
        hit = idx[:, k][None, :] == e[:, None]
        flat.append(jnp.sum(jnp.where(hit, (e ^ me)[:, None] * cap + slot, 0), axis=0))
    flat = jnp.stack(flat, axis=1)
    vm = pl.BlockSpec(memory_space=pltpu.VMEM)
    hb = pl.BlockSpec(memory_space=pl.ANY)
    bf = jnp.bfloat16
    ff = w2.shape[0]
    return pl.pallas_call(
        functools.partial(moe_kernel, ne, cap),
        in_specs=[vm, vm, vm, vm, hb, hb, hb], out_specs=vm,
        out_shape=jax.ShapeDtypeStruct((t, hd), bf),
        scratch_shapes=[pltpu.VMEM((ne, cap, hd), bf), pltpu.VMEM((ne, cap, hd), bf), pltpu.VMEM((NEAR * cap, ff), bf),
                        pltpu.VMEM((ne, cap, hd), bf), pltpu.VMEM((ne, cap, hd), bf), pltpu.VMEM((2 * t, ne * cap), bf),
                        pltpu.VMEM((2, 2, hd, FT), bf), pltpu.VMEM((2, ff, NT), bf)]
                       + [pltpu.SemaphoreType.DMA((ne,))] * 4 + [pltpu.SemaphoreType.DMA((2, 2)), pltpu.SemaphoreType.DMA((2,))],
        compiler_params=pltpu.CompilerParams(collective_id=cid, has_side_effects=True, vmem_limit_bytes=63 * 1024 * 1024),
        name='moe')(h, slot, flat, gates, w1g, w1u, w2)


def expert_ffn(rows, wg, wu, wd):
    gg = jnp.dot(rows, wg, preferred_element_type=jnp.float32)
    uu = jnp.dot(rows, wu, preferred_element_type=jnp.float32)
    act = (jax.nn.silu(gg) * uu).astype(jnp.bfloat16)
    return jnp.dot(act, wd, preferred_element_type=jnp.float32).astype(jnp.bfloat16)


def attention_residual(x, wq, wk, wv, wo, cp):
    xs = lax.all_gather(x, 'tp', axis=0, tiled=True)
    seg = xs.shape[0] // 2
    wkv = jnp.concatenate([wk, wv], axis=1)
    kv = jnp.dot(xs, wkv, preferred_element_type=jnp.float32).astype(jnp.bfloat16)
    kvs = lax.all_gather(kv, 'cp', axis=0)
    q = jnp.dot(xs, wq, preferred_element_type=jnp.float32).astype(jnp.bfloat16)
    kvp = jnp.concatenate([kvs[r, :seg] for r in range(cp)] + [kvs[r, seg:] for r in reversed(range(cp))], axis=0)
    o = attention(q, kvp, cp)
    part = jnp.dot(o, wo, preferred_element_type=jnp.float32)
    att = lax.psum_scatter(part, 'tp', scatter_dimension=0, tiled=True)
    return (x.astype(jnp.float32) + att).astype(jnp.bfloat16)


def routing(idx, ne):
    t = idx.shape[0]
    it = idx.T
    hit = (it[0][None, :] == jnp.arange(ne)[:, None]) | (it[1][None, :] == jnp.arange(ne)[:, None])
    before = (jnp.arange(t)[:, None] < jnp.arange(t)[None, :]).astype(jnp.bfloat16)
    rank = jnp.dot(hit.astype(jnp.bfloat16), before, preferred_element_type=jnp.float32).astype(jnp.int32)
    return jnp.where(hit, rank, -1)


def moe_any(h, slot, idx, gates, wg, wu, wd):
    t, hd = h.shape
    ne = slot.shape[0]
    cap = 4 * t // ne
    pick = (slot[:, None, :] == jnp.arange(cap)[None, :, None]).astype(jnp.bfloat16).reshape(ne * cap, t)
    send = jnp.dot(pick, h, preferred_element_type=jnp.float32).astype(jnp.bfloat16)
    recv = lax.all_to_all(send.reshape(ne, cap, hd), ('cp', 'tp'), 0, 0, tiled=True)
    z = expert_ffn(recv.reshape(ne * cap, hd), wg, wu, wd)
    back = lax.all_to_all(z.reshape(ne, cap, hd), ('cp', 'tp'), 0, 0, tiled=True).reshape(ne * cap, hd)
    flat = jnp.arange(ne * cap)
    y = h.astype(jnp.float32)
    for k in range(2):
        mine = jnp.sum(jnp.where(idx[:, k][None, :] == jnp.arange(ne)[:, None], jnp.arange(ne)[:, None] * cap + slot, 0), axis=0)
        sel = (mine[:, None] == flat[None, :]).astype(jnp.bfloat16)
        y = y + gates[:, k:k + 1] * jnp.dot(sel, back, preferred_element_type=jnp.float32)
    return y.astype(jnp.bfloat16)


def solution(mesh):
    cp = mesh.shape['cp']
    tp = mesh.shape['tp']
    ne = cp * tp
    rows_spec = P(('dp', 'cp', 'tp'), None)
    exp_spec = P(('cp', 'tp'), None, None)

    def local(x, idx, gates, wq, wk, wv, wo, w1g, w1u, w2):
        t, hd = x.shape
        slot = routing(idx, ne)
        h = attention_residual(x, wq, wk, wv, wo, cp)
        count = jnp.max(jnp.sum((slot >= 0).astype(jnp.int32), axis=1))
        worst = lax.pmax(count, ('cp', 'tp'))

        def tight(h):
            return moe_fast(h, slot, idx, gates, w1g[0], w1u[0], w2[0], t // 4, 3)

        def roomy(h):
            return moe_any(h, slot, idx, gates, w1g[0], w1u[0], w2[0])

        return lax.cond(worst <= t // 4, tight, roomy, h)

    return jax.shard_map(local, mesh=mesh, in_specs=(rows_spec, rows_spec, rows_spec, P(None, 'tp'), P(None, 'tp'), P(None, 'tp'), P('tp', None), exp_spec, exp_spec, exp_spec), out_specs=rows_spec, check_vma=False)
```

```python
import functools
import math

import jax
import jax.numpy as jnp
from jax import lax
from jax.experimental import pallas as pl
from jax.experimental.pallas import tpu as pltpu
from jax.sharding import PartitionSpec as P


MESH = pl.DeviceIdType.MESH
NEAR = 6
FT = 256
NT = 512


def peer(r):
    c, t = lax.axis_index('cp'), lax.axis_index('tp')
    core, xx = lax.rem(t, 2), t // 2
    core = 1 - core if r & 1 else core
    xx = 1 - xx if r & 2 else xx
    c = 1 - c if r & 4 else c
    return c, xx * 2 + core


def device(r):
    c, t = peer(r)
    return (lax.axis_index('dp'), c, t)


def greet(peers):
    bar = pltpu.get_barrier_semaphore()
    for r in peers:
        pl.semaphore_signal(bar, inc=1, device_id=device(r), device_id_type=MESH)
    pl.semaphore_wait(bar, len(peers))


def moe_kernel(ne, cap, h_ref, slot_ref, flat_ref, gate_ref, w1g_ref, w1u_ref, w2_ref, y_ref,
               send, recv, act, zsend, zrecv, pick, w1b, w2b, ds, dr, zs, zr, w1s, w2s):
    t, hd = h_ref.shape
    ff = w2_ref.shape[0]
    nf, nz = ff // FT, hd // NT

    def w1_copy(tile, slot, which):
        src = (w1g_ref, w1u_ref)[which]
        return pltpu.make_async_copy(src.at[:, pl.ds(pl.multiple_of(tile * FT, FT), FT)], w1b.at[slot, which], w1s.at[slot, which])

    def w2_copy(tile, slot):
        return pltpu.make_async_copy(w2_ref.at[:, pl.ds(pl.multiple_of(tile * NT, NT), NT)], w2b.at[slot], w2s.at[slot])

    for s in range(2):
        w1_copy(s, s, 0).start()
        w1_copy(s, s, 1).start()
    for s in range(2):
        w2_copy(s, s).start()

    def out_copy(r):
        return pltpu.make_async_remote_copy(src_ref=send.at[r], dst_ref=recv.at[r], send_sem=ds.at[r], recv_sem=dr.at[r], device_id=device(r), device_id_type=MESH)

    def dispatch(r, dst):
        c, tt = peer(r)
        row = slot_ref[pl.ds(c * (ne // 2) + tt, 1), :]
        sel = (jnp.broadcast_to(row, (cap, t)) == lax.broadcasted_iota(jnp.int32, (cap, t), 0)).astype(jnp.bfloat16)

        def tile(n, _):
            cols = pl.ds(pl.multiple_of(n * NT, NT), NT)
            dst[r, :, cols] = jnp.dot(sel, h_ref[:, cols], preferred_element_type=jnp.float32).astype(jnp.bfloat16)
            return 0
        lax.fori_loop(0, nz, tile, 0)

    order = (2, 4, 3, 5, 6, 7, 1)
    dispatch(order[0], send)
    greet(range(1, ne))
    for a, r in enumerate(order):
        if a + 1 < len(order):
            dispatch(order[a + 1], send)
        else:
            dispatch(0, recv)
        out_copy(r).start()
    for k in range(2):
        pick[k * t:(k + 1) * t, :] = (flat_ref[:, k:k + 1] == lax.broadcasted_iota(jnp.int32, (t, ne * cap), 1)).astype(jnp.bfloat16)

    def back_copy(r, tile):
        cols = pl.ds(pl.multiple_of(tile * NT, NT), NT)
        return pltpu.make_async_remote_copy(src_ref=zsend.at[r, :, cols], dst_ref=zrecv.at[r, :, cols], send_sem=zs.at[r], recv_sem=zr.at[r], device_id=device(r), device_id_type=MESH)

    def experts(lo, hi, again):
        rows = (hi - lo) * cap
        off = 0 if again else nz

        def up(f, _):
            slot = lax.rem(f, 2)
            w1_copy(f, slot, 0).wait()
            w1_copy(f, slot, 1).wait()
            xr = recv[lo:hi].reshape(rows, hd)
            gg = jnp.dot(xr, w1b[slot, 0], preferred_element_type=jnp.float32)
            uu = jnp.dot(xr, w1b[slot, 1], preferred_element_type=jnp.float32)
            act[:rows, pl.ds(pl.multiple_of(f * FT, FT), FT)] = (gg * jax.nn.sigmoid(gg) * uu).astype(jnp.bfloat16)
            nxt = f + 2

            @pl.when(nxt < (nf + 2 if again else nf))
            def _():
                w1_copy(lax.rem(nxt, nf), slot, 0).start()
                w1_copy(lax.rem(nxt, nf), slot, 1).start()
            return 0
        lax.fori_loop(0, nf, up, 0)

        def down(n, _):
            slot = lax.rem(n + off, 2)
            w2_copy(n, slot).wait()

            @pl.when(n > 0)
            def _():
                for r in range(max(lo, 1), hi):
                    back_copy(r, n - 1).start()
            zz = jnp.dot(act[:rows], w2b[slot], preferred_element_type=jnp.float32).astype(jnp.bfloat16)
            cols = pl.ds(pl.multiple_of(n * NT, NT), NT)
            for r in range(lo, hi):
                dst = zrecv if r == 0 else zsend
                dst[r, :, cols] = zz[(r - lo) * cap:(r - lo + 1) * cap]
            nxt = n + 2

            @pl.when(nxt < (nz + 2 if again else nz))
            def _():
                w2_copy(lax.rem(nxt, nz), slot).start()
            return 0
        lax.fori_loop(0, nz, down, 0)
        for r in range(max(lo, 1), hi):
            back_copy(r, nz - 1).start()

    for r in range(1, NEAR):
        out_copy(r).wait_recv()
    experts(0, NEAR, True)
    for r in range(NEAR, ne):
        out_copy(r).wait_recv()
    experts(NEAR, ne, False)
    whole = lambda r: pltpu.make_async_remote_copy(src_ref=zsend.at[r], dst_ref=zrecv.at[r], send_sem=zs.at[r], recv_sem=zr.at[r], device_id=device(r), device_id_type=MESH)
    for r in range(1, ne):
        whole(r).wait_recv()

    def combine(n, _):
        cols = pl.ds(pl.multiple_of(n * NT, NT), NT)
        zt = jnp.dot(pick[...], zrecv[:, :, cols].reshape(ne * cap, NT), preferred_element_type=jnp.float32)
        y = h_ref[:, cols].astype(jnp.float32) + (gate_ref[:, 0:1] * zt[:t] + gate_ref[:, 1:2] * zt[t:])
        y_ref[:, cols] = y.astype(jnp.bfloat16)
        return 0
    lax.fori_loop(0, nz, combine, 0)
    for r in range(1, ne):
        out_copy(r).wait_send()
        whole(r).wait_send()


def moe_fast(h, slot, idx, gates, w1g, w1u, w2, cap, cid):
    t, hd = h.shape
    ne = slot.shape[0]
    me = lax.axis_index('cp') * (ne // 2) + lax.axis_index('tp')
    e = jnp.arange(ne)
    flat = []
    for k in range(2):
        hit = idx[:, k][None, :] == e[:, None]
        flat.append(jnp.sum(jnp.where(hit, (e ^ me)[:, None] * cap + slot, 0), axis=0))
    flat = jnp.stack(flat, axis=1)
    vm = pl.BlockSpec(memory_space=pltpu.VMEM)
    hb = pl.BlockSpec(memory_space=pl.ANY)
    bf = jnp.bfloat16
    ff = w2.shape[0]
    return pl.pallas_call(
        functools.partial(moe_kernel, ne, cap),
        in_specs=[vm, vm, vm, vm, hb, hb, hb], out_specs=vm,
        out_shape=jax.ShapeDtypeStruct((t, hd), bf),
        scratch_shapes=[pltpu.VMEM((ne, cap, hd), bf), pltpu.VMEM((ne, cap, hd), bf), pltpu.VMEM((NEAR * cap, ff), bf),
                        pltpu.VMEM((ne, cap, hd), bf), pltpu.VMEM((ne, cap, hd), bf), pltpu.VMEM((2 * t, ne * cap), bf),
                        pltpu.VMEM((2, 2, hd, FT), bf), pltpu.VMEM((2, ff, NT), bf)]
                       + [pltpu.SemaphoreType.DMA((ne,))] * 4 + [pltpu.SemaphoreType.DMA((2, 2)), pltpu.SemaphoreType.DMA((2,))],
        compiler_params=pltpu.CompilerParams(collective_id=cid, has_side_effects=True, vmem_limit_bytes=63 * 1024 * 1024),
        name='moe')(h, slot, flat, gates, w1g, w1u, w2)


D = 128
PIECES = 4
CHUNKS = 4
HOOKS = (6, 12)


def mate(r):
    t = lax.axis_index('tp')
    core = lax.rem(lax.rem(t, 2) + lax.rem(r, 2), 2)
    xx = lax.rem(t // 2 + r // 2, 2)
    return xx * 2 + core


def segment(t, cp):
    c = lax.axis_index('cp')
    return jnp.where(t < 2, c, 2 * cp - 1 - c)


def remote(src, dst, send, recv, dev):
    return pltpu.make_async_remote_copy(src_ref=src, dst_ref=dst, send_sem=send, recv_sem=recv, device_id=dev, device_id_type=MESH)


def qkv_kernel(cp, ne, x_ref, cnt_ref, wq_ref, wk_ref, wv_ref, q_ref, kv_ref, all_ref,
               xs, wqb, wkvb, cs, cr, xsnd, xrcv, fs, fr, bs, br, ks, kr, ws):
    t = x_ref.shape[0]
    step = t // PIECES
    loads = [pltpu.make_async_copy(wk_ref, wkvb.at[:, :D], ws.at[0]), pltpu.make_async_copy(wv_ref, wkvb.at[:, D:], ws.at[1]),
             pltpu.make_async_copy(wq_ref, wqb, ws.at[2])]
    for ld in loads:
        ld.start()
    greet(range(1, ne))
    counts = [remote(cnt_ref, all_ref.at[r], cs.at[r], cr.at[r], device(r)) for r in range(1, ne)]
    for cc in counts:
        cc.start()
    rows = lambda p: pl.ds(p * step, step)
    across = [remote(x_ref.at[rows(p)], xs.at[1, rows(p)], xsnd.at[p], xrcv.at[p], device(2)) for p in range(PIECES)]
    for a in across:
        a.start()
    beside = remote(x_ref, xs.at[0], bs.at[0], br.at[0], device(1))
    beside.start()
    onward = [remote(xs.at[1, rows(p)], xs.at[2, rows(p)], fs.at[p], fr.at[p], device(1)) for p in range(PIECES)]
    all_ref[0] = cnt_ref[...]
    for ld in loads:
        ld.wait()
    sent = []

    def project(block, r, off, n):
        tt = mate(r)
        base = pl.multiple_of(segment(tt, cp) * (2 * t) + lax.rem(tt, 2) * t + off, 16)
        kv_ref[pl.ds(base, n), :] = jnp.dot(block, wkvb[...], preferred_element_type=jnp.float32).astype(jnp.bfloat16)
        qb = pl.multiple_of(tt * t + off, 16)
        q_ref[pl.ds(qb, n), :] = jnp.dot(block, wqb[...], preferred_element_type=jnp.float32).astype(jnp.bfloat16)
        i = len(sent)
        out = remote(kv_ref.at[pl.ds(base, n)], kv_ref.at[pl.ds(base, n)], ks.at[i], kr.at[i], device(4))
        out.start()
        sent.append(out)

    project(x_ref[...], 0, 0, t)
    beside.wait_recv()
    project(xs[0], 1, 0, t)
    for p in range(PIECES):
        across[p].wait_recv()
        onward[p].start()
        project(xs[1, p * step:(p + 1) * step], 2, p * step, step)
        onward[p].wait_recv()
        project(xs[2, p * step:(p + 1) * step], 3, p * step, step)
    for o in sent:
        o.wait_recv()
    for cc in counts:
        cc.wait_recv()
    for o in counts + across + [beside] + onward + sent:
        o.wait_send()


def qkv(x, cnt, wq, wk, wv, cp, ne, cid):
    t, hd = x.shape
    tp = ne // cp
    vm = pl.BlockSpec(memory_space=pltpu.VMEM)
    hb = pl.BlockSpec(memory_space=pl.ANY)
    bf = jnp.bfloat16
    dma = pltpu.SemaphoreType.DMA
    nk = 2 + 2 * PIECES
    return pl.pallas_call(
        functools.partial(qkv_kernel, cp, ne),
        in_specs=[vm, vm, hb, hb, hb], out_specs=[vm, vm, vm],
        out_shape=[jax.ShapeDtypeStruct((tp * t, wq.shape[1]), bf), jax.ShapeDtypeStruct((ne * t, 2 * D), bf), jax.ShapeDtypeStruct((ne,) + cnt.shape, jnp.int32)],
        scratch_shapes=[pltpu.VMEM((3, t, hd), bf), pltpu.VMEM(wq.shape, bf), pltpu.VMEM((hd, 2 * D), bf),
                        dma((ne,)), dma((ne,)), dma((PIECES,)), dma((PIECES,)), dma((PIECES,)), dma((PIECES,)), dma((1,)), dma((1,)), dma((nk,)), dma((nk,)), dma((3,))],
        compiler_params=pltpu.CompilerParams(collective_id=cid, has_side_effects=True, vmem_limit_bytes=60 * 1024 * 1024),
        name='qkv')(x, cnt, wq, wk, wv)


def attn_kernel(cp, q_ref, kv_ref, x_ref, wo_ref, h_ref, wof, ocat, obuf, m_ref, l_ref, acc_ref, part,
                xs_, xr_, ys_, yr_, ds_, dr_, os_, or_, ls_):
    t, hd = x_ref.shape
    w = wo_ref.shape[0]
    heads = w // D
    half = w // 2
    step = half // CHUNKS
    c = lax.axis_index('cp')
    mine = pltpu.make_async_copy(wo_ref, wof.at[:w], ls_.at[0])
    mine.start()
    greet((1, 2, 3, 4))
    at = lambda base, j: pl.ds(pl.multiple_of(base + j * step, 16), step)
    first, second = c * half, (1 - c) * half
    xc = [remote(wo_ref.at[at(first, j)], wof.at[at(2 * w + first, j)], xs_.at[j], xr_.at[j], device(2)) for j in range(CHUNKS)]
    yc = [remote(wof.at[at(2 * w + first, j)], wof.at[at(2 * w + first, j)], ys_.at[j], yr_.at[j], device(4)) for j in range(CHUNKS)]
    dx = [remote(wof.at[at(2 * w + first, j)], wof.at[at(3 * w + first, j)], ds_.at[j], dr_.at[j], device(1)) for j in range(CHUNKS)]
    dy = [remote(wof.at[at(2 * w + second, j)], wof.at[at(3 * w + second, j)], ds_.at[CHUNKS + j], dr_.at[CHUNKS + j], device(1)) for j in range(CHUNKS)]
    whole = remote(wo_ref, wof.at[pl.ds(w, w)], ds_.at[2 * CHUNKS], dr_.at[2 * CHUNKS], device(1))
    for cpy in xc:
        cpy.start()
    whole.start()

    def relay_x(j):
        xc[j].wait_recv()
        yc[j].start()
        dx[j].start()

    def relay_y(j):
        yc[j].wait_recv()
        dy[j].start()

    scale = D ** -0.5 * math.log2(math.e)
    mask = lax.broadcasted_iota(jnp.int32, (t, t), 1) <= lax.broadcasted_iota(jnp.int32, (t, t), 0)

    def lanes(p):
        s = p[:, :128]
        for a in range(128, t, 128):
            s = s + p[:, a:a + 128]
        return s

    def which(b):
        return jnp.where(b < 2, b + 2, 3 - b)

    def give(b):
        r = which(b)
        return remote(obuf.at[r], ocat.at[:, pl.ds(pl.multiple_of(r * w, 128), w)], os_.at[r], or_.at[r], (lax.axis_index('dp'), c, mate(r)))

    def block(b, u):
        r = which(b)
        tt = mate(r)
        qb = pl.multiple_of(tt * t, t)
        nfull = segment(tt, cp) * 2 + lax.rem(tt, 2)

        def scores(h, j):
            k = kv_ref[pl.ds(pl.multiple_of(j * t, t), t), :D]
            q = q_ref[pl.ds(qb, t), h * D:(h + 1) * D]
            return lax.dot_general(q, k, (((1,), (1,)), ((), ())), preferred_element_type=jnp.float32) * scale

        def pv(p, j):
            v = kv_ref[pl.ds(pl.multiple_of(j * t, t), t), D:]
            return jnp.dot(p.astype(jnp.bfloat16), v, preferred_element_type=jnp.float32)

        for h in range(heads):
            s = jnp.where(mask, scores(h, nfull), -1e30)
            m = jnp.max(s, axis=1, keepdims=True)
            p = jnp.where(mask, jnp.exp2(s - m), 0.0)
            m_ref[h] = jnp.broadcast_to(m, (t, 128))
            l_ref[h] = lanes(p)
            acc_ref[h] = pv(p, nfull)

        @pl.when(b > 0)
        def _():
            give(b - 1).start()

        def body(j, _):
            for n, at_unit in enumerate(HOOKS):
                @pl.when(u + j == at_unit)
                def _():
                    relay_x(n)
            for h in range(heads):
                s = scores(h, j)
                mo = m_ref[h]
                mn = jnp.maximum(mo, jnp.max(s, axis=1, keepdims=True))
                p = jnp.exp2(s - jnp.concatenate([mn] * (t // 128), axis=1))
                al = jnp.exp2(mo - mn)
                m_ref[h] = mn
                l_ref[h] = l_ref[h] * al + lanes(p)
                acc_ref[h] = acc_ref[h] * al + pv(p, j)
            return 0

        lax.fori_loop(0, nfull, body, 0)
        for h in range(heads):
            l = jnp.sum(l_ref[h], axis=1, keepdims=True)
            obuf[r, :, h * D:(h + 1) * D] = (acc_ref[h] / l).astype(jnp.bfloat16)
        return u + nfull

    units = lax.fori_loop(0, 4, block, 0)
    ocat[:, :w] = obuf[0]
    mine.wait()
    whole.wait_recv()
    give(2).wait_recv()

    def near(n, _):
        cols = pl.ds(pl.multiple_of(n * NT, NT), NT)
        part[:, cols] = jnp.dot(ocat[:, :2 * w], wof[:2 * w, cols], preferred_element_type=jnp.float32)
        return 0
    lax.fori_loop(0, hd // NT, near, 0)
    relay_x(2)
    relay_y(0)
    relay_x(3)
    relay_y(1)
    relay_y(2)
    relay_y(3)
    for j in range(CHUNKS):
        dx[j].wait_recv()
        dy[j].wait_recv()
    give(0).wait_recv()
    give(1).wait_recv()

    def far(n, _):
        cols = pl.ds(pl.multiple_of(n * NT, NT), NT)
        s = part[:, cols] + jnp.dot(ocat[:, 2 * w:], wof[2 * w:, cols], preferred_element_type=jnp.float32)
        h_ref[:, cols] = (x_ref[:, cols].astype(jnp.float32) + s).astype(jnp.bfloat16)
        return 0
    lax.fori_loop(0, hd // NT, far, 0)
    for cpy in xc + yc + dx + dy + [whole, give(0), give(1), give(2)]:
        cpy.wait_send()


def attention(q, kv, x, wo, cp, cid):
    t, hd = x.shape
    w = wo.shape[0]
    heads = w // D
    vm = pl.BlockSpec(memory_space=pltpu.VMEM)
    hb = pl.BlockSpec(memory_space=pl.ANY)
    bf = jnp.bfloat16
    dma = pltpu.SemaphoreType.DMA
    state = pltpu.VMEM((heads, t, 128), jnp.float32)
    return pl.pallas_call(
        functools.partial(attn_kernel, cp),
        in_specs=[vm, vm, vm, hb], out_specs=vm,
        out_shape=jax.ShapeDtypeStruct((t, hd), bf),
        scratch_shapes=[pltpu.VMEM((4 * w, hd), bf), pltpu.VMEM((t, 4 * w), bf), pltpu.VMEM((4, t, w), bf), state, state, state, pltpu.VMEM((t, hd), jnp.float32),
                        dma((CHUNKS,)), dma((CHUNKS,)), dma((CHUNKS,)), dma((CHUNKS,)), dma((2 * CHUNKS + 1,)), dma((2 * CHUNKS + 1,)), dma((4,)), dma((4,)), dma((1,))],
        compiler_params=pltpu.CompilerParams(collective_id=cid, has_side_effects=True, vmem_limit_bytes=63 * 1024 * 1024),
        name='attn')(q, kv, x, wo)


def expert_ffn(rows, wg, wu, wd):
    gg = jnp.dot(rows, wg, preferred_element_type=jnp.float32)
    uu = jnp.dot(rows, wu, preferred_element_type=jnp.float32)
    act = (jax.nn.silu(gg) * uu).astype(jnp.bfloat16)
    return jnp.dot(act, wd, preferred_element_type=jnp.float32).astype(jnp.bfloat16)


def routing(idx, ne):
    t = idx.shape[0]
    it = idx.T
    hit = (it[0][None, :] == jnp.arange(ne)[:, None]) | (it[1][None, :] == jnp.arange(ne)[:, None])
    before = (jnp.arange(t)[:, None] < jnp.arange(t)[None, :]).astype(jnp.bfloat16)
    rank = jnp.dot(hit.astype(jnp.bfloat16), before, preferred_element_type=jnp.float32).astype(jnp.int32)
    return jnp.where(hit, rank, -1)


def moe_any(h, slot, idx, gates, wg, wu, wd):
    t, hd = h.shape
    ne = slot.shape[0]
    cap = 4 * t // ne
    pick = (slot[:, None, :] == jnp.arange(cap)[None, :, None]).astype(jnp.bfloat16).reshape(ne * cap, t)
    send = jnp.dot(pick, h, preferred_element_type=jnp.float32).astype(jnp.bfloat16)
    recv = lax.all_to_all(send.reshape(ne, cap, hd), ('cp', 'tp'), 0, 0, tiled=True)
    z = expert_ffn(recv.reshape(ne * cap, hd), wg, wu, wd)
    back = lax.all_to_all(z.reshape(ne, cap, hd), ('cp', 'tp'), 0, 0, tiled=True).reshape(ne * cap, hd)
    flat = jnp.arange(ne * cap)
    y = h.astype(jnp.float32)
    for k in range(2):
        mine = jnp.sum(jnp.where(idx[:, k][None, :] == jnp.arange(ne)[:, None], jnp.arange(ne)[:, None] * cap + slot, 0), axis=0)
        sel = (mine[:, None] == flat[None, :]).astype(jnp.bfloat16)
        y = y + gates[:, k:k + 1] * jnp.dot(sel, back, preferred_element_type=jnp.float32)
    return y.astype(jnp.bfloat16)


def solution(mesh):
    cp = mesh.shape['cp']
    tp = mesh.shape['tp']
    ne = cp * tp
    rows_spec = P(('dp', 'cp', 'tp'), None)
    exp_spec = P(('cp', 'tp'), None, None)

    def local(x, idx, gates, wq, wk, wv, wo, w1g, w1u, w2):
        t, hd = x.shape
        slot = routing(idx, ne)
        counts = jnp.broadcast_to(jnp.sum((slot >= 0).astype(jnp.int32), axis=1)[:, None], (ne, D))
        q, kv, counts = qkv(x, counts, wq, wk, wv, cp, ne, 1)
        h = attention(q, kv, x, wo, cp, 2)
        worst = jnp.max(counts)

        def tight(h):
            return moe_fast(h, slot, idx, gates, w1g[0], w1u[0], w2[0], t // 4, 3)

        def roomy(h):
            return moe_any(h, slot, idx, gates, w1g[0], w1u[0], w2[0])

        return lax.cond(worst <= t // 4, tight, roomy, h)

    return jax.shard_map(local, mesh=mesh, in_specs=(rows_spec, rows_spec, rows_spec, P(None, 'tp'), P(None, 'tp'), P(None, 'tp'), P('tp', None), exp_spec, exp_spec, exp_spec), out_specs=rows_spec, check_vma=False)
```

```python
import functools
import math

import jax
import jax.numpy as jnp
from jax import lax
from jax.experimental import pallas as pl
from jax.experimental.pallas import tpu as pltpu
from jax.sharding import PartitionSpec as P


MESH = pl.DeviceIdType.MESH
NEAR = 6
FT = 512
NT = 512


def peer(r):
    c, t = lax.axis_index('cp'), lax.axis_index('tp')
    core, xx = lax.rem(t, 2), t // 2
    core = 1 - core if r & 1 else core
    xx = 1 - xx if r & 2 else xx
    c = 1 - c if r & 4 else c
    return c, xx * 2 + core


def device(r):
    c, t = peer(r)
    return (lax.axis_index('dp'), c, t)


def hail(peers):
    bar = pltpu.get_barrier_semaphore()
    for r in peers:
        pl.semaphore_signal(bar, inc=1, device_id=device(r), device_id_type=MESH)


def greet(peers):
    hail(peers)
    pl.semaphore_wait(pltpu.get_barrier_semaphore(), len(peers))


def moe_kernel(ne, cap, h_ref, slot_ref, meta_ref, w1g_ref, w1u_ref, w2_ref, y_ref,
               send, recv, act, zsend, zrecv, sel, pick, w1b, w2b, ds, dr, zs, zr, zf, w1s, w2s):
    t, hd = h_ref.shape
    ff = w2_ref.shape[0]
    nf, nz = ff // FT, hd // NT

    def w1_copy(tile, slot, which):
        src = (w1g_ref, w1u_ref)[which]
        return pltpu.make_async_copy(src.at[:, pl.ds(pl.multiple_of(tile * FT, FT), FT)], w1b.at[slot, which], w1s.at[slot, which])

    def w2_copy(tile, slot):
        return pltpu.make_async_copy(w2_ref.at[:, pl.ds(pl.multiple_of(tile * NT, NT), NT)], w2b.at[slot], w2s.at[slot])

    for s in range(2):
        w1_copy(s, s, 0).start()
        w1_copy(s, s, 1).start()
    for s in range(2):
        w2_copy(s, s).start()

    hail(range(1, ne))
    tile = lambda n: pl.ds(pl.multiple_of(n * NT, NT), NT)

    def out_copy(r, cols=slice(None)):
        return pltpu.make_async_remote_copy(src_ref=send.at[r, :, cols], dst_ref=recv.at[r, :, cols], send_sem=ds.at[r], recv_sem=dr.at[r], device_id=device(r), device_id_type=MESH)

    for r in range(ne):
        c, tt = peer(r)
        row = slot_ref[pl.ds(c * (ne // 2) + tt, 1), :]
        sel[r * cap:(r + 1) * cap, :] = (jnp.broadcast_to(row, (cap, t)) == lax.broadcasted_iota(jnp.int32, (cap, t), 0)).astype(jnp.bfloat16)
    pl.semaphore_wait(pltpu.get_barrier_semaphore(), ne - 1)

    def dispatch(lo, hi, order):
        def one(n, _):
            rows = jnp.dot(sel[lo * cap:hi * cap, :], h_ref[:, tile(n)], preferred_element_type=jnp.float32).astype(jnp.bfloat16)
            for r in range(lo, hi):
                dst = recv if r == 0 else send
                dst[r, :, tile(n)] = rows[(r - lo) * cap:(r - lo + 1) * cap]

            @pl.when(n > 0)
            def _():
                for r in order:
                    out_copy(r, tile(n - 1)).start()
            return 0
        lax.fori_loop(0, nz, one, 0)
        for r in order:
            out_copy(r, tile(nz - 1)).start()

    dispatch(0, NEAR, (2, 4, 3, 5, 1))
    dispatch(NEAR, ne, (6, 7))
    for k in range(2):
        pick[k * t:(k + 1) * t, :] = (meta_ref[:, k:k + 1] == lax.broadcasted_iota(jnp.int32, (t, ne * cap), 1).astype(jnp.float32)).astype(jnp.bfloat16)

    def back_copy(r, n):
        got = zr.at[r] if r < NEAR else zf.at[r - NEAR, n]
        return pltpu.make_async_remote_copy(src_ref=zsend.at[r, :, tile(n)], dst_ref=zrecv.at[r, :, tile(n)], send_sem=zs.at[r], recv_sem=got, device_id=device(r), device_id_type=MESH)

    def experts(lo, hi, again):
        rows = (hi - lo) * cap
        off, off1 = (0, 0) if again else (nz, nf)

        def up(f, _):
            slot = lax.rem(f + off1, 2)
            w1_copy(f, slot, 0).wait()
            w1_copy(f, slot, 1).wait()
            xr = recv[lo:hi].reshape(rows, hd)
            gg = jnp.dot(xr, w1b[slot, 0], preferred_element_type=jnp.float32)
            uu = jnp.dot(xr, w1b[slot, 1], preferred_element_type=jnp.float32)
            act[:rows, pl.ds(pl.multiple_of(f * FT, FT), FT)] = (gg * jax.nn.sigmoid(gg) * uu).astype(jnp.bfloat16)
            nxt = f + 2

            @pl.when(nxt < (nf + 2 if again else nf))
            def _():
                w1_copy(lax.rem(nxt, nf), slot, 0).start()
                w1_copy(lax.rem(nxt, nf), slot, 1).start()
            return 0
        lax.fori_loop(0, nf, up, 0)

        def down(n, _):
            slot = lax.rem(n + off, 2)
            w2_copy(n, slot).wait()

            @pl.when(n > 0)
            def _():
                for r in range(max(lo, 1), hi):
                    back_copy(r, n - 1).start()
            zz = jnp.dot(act[:rows], w2b[slot], preferred_element_type=jnp.float32).astype(jnp.bfloat16)
            cols = pl.ds(pl.multiple_of(n * NT, NT), NT)
            for r in range(lo, hi):
                dst = zrecv if r == 0 else zsend
                dst[r, :, cols] = zz[(r - lo) * cap:(r - lo + 1) * cap]
            nxt = n + 2

            @pl.when(nxt < (nz + 2 if again else nz))
            def _():
                w2_copy(lax.rem(nxt, nz), slot).start()
            return 0
        lax.fori_loop(0, nz, down, 0)
        for r in range(max(lo, 1), hi):
            back_copy(r, nz - 1).start()

    for r in range(1, NEAR):
        out_copy(r).wait_recv()
    experts(0, NEAR, True)
    for r in range(NEAR, ne):
        out_copy(r).wait_recv()
    experts(NEAR, ne, False)
    whole = lambda r: pltpu.make_async_remote_copy(src_ref=zsend.at[r], dst_ref=zrecv.at[r], send_sem=zs.at[r], recv_sem=zr.at[r], device_id=device(r), device_id_type=MESH)
    for r in range(1, NEAR):
        whole(r).wait_recv()

    def combine(n, _):
        cols = tile(n)
        for r in range(NEAR, ne):
            back_copy(r, n).wait_recv()
        zt = jnp.dot(pick[...], zrecv[:, :, cols].reshape(ne * cap, NT), preferred_element_type=jnp.float32)
        y = h_ref[:, cols].astype(jnp.float32) + (meta_ref[:, 2:3] * zt[:t] + meta_ref[:, 3:4] * zt[t:])
        y_ref[:, cols] = y.astype(jnp.bfloat16)
        return 0
    lax.fori_loop(0, nz, combine, 0)
    for r in range(1, ne):
        out_copy(r).wait_send()
        whole(r).wait_send()


def moe_fast(h, slot, meta, w1g, w1u, w2, cap, cid):
    t, hd = h.shape
    ne = slot.shape[0]
    vm = pl.BlockSpec(memory_space=pltpu.VMEM)
    hb = pl.BlockSpec(memory_space=pl.ANY)
    bf = jnp.bfloat16
    ff = w2.shape[0]
    return pl.pallas_call(
        functools.partial(moe_kernel, ne, cap),
        in_specs=[vm, vm, vm, hb, hb, hb], out_specs=vm,
        out_shape=jax.ShapeDtypeStruct((t, hd), bf),
        scratch_shapes=[pltpu.VMEM((ne, cap, hd), bf), pltpu.VMEM((ne, cap, hd), bf), pltpu.VMEM((NEAR * cap, ff), bf),
                        pltpu.VMEM((ne, cap, hd), bf), pltpu.VMEM((ne, cap, hd), bf), pltpu.VMEM((ne * cap, t), bf), pltpu.VMEM((2 * t, ne * cap), bf),
                        pltpu.VMEM((2, 2, hd, FT), bf), pltpu.VMEM((2, ff, NT), bf)]
                       + [pltpu.SemaphoreType.DMA((ne,))] * 4 + [pltpu.SemaphoreType.DMA((ne - NEAR, hd // NT))] + [pltpu.SemaphoreType.DMA((2, 2)), pltpu.SemaphoreType.DMA((2,))],
        compiler_params=pltpu.CompilerParams(collective_id=cid, has_side_effects=True, vmem_limit_bytes=63 * 1024 * 1024),
        name='moe')(h, slot, meta, w1g, w1u, w2)


D = 128
PIECES = 4
CHUNKS = 4
HOOKS = (6, 12)


def mate(r):
    t = lax.axis_index('tp')
    core = lax.rem(lax.rem(t, 2) + lax.rem(r, 2), 2)
    xx = lax.rem(t // 2 + r // 2, 2)
    return xx * 2 + core


def segment(t, cp):
    c = lax.axis_index('cp')
    return jnp.where(t < 2, c, 2 * cp - 1 - c)


def remote(src, dst, send, recv, dev):
    return pltpu.make_async_remote_copy(src_ref=src, dst_ref=dst, send_sem=send, recv_sem=recv, device_id=dev, device_id_type=MESH)


def qkv_kernel(cp, ne, x_ref, idx_ref, gate_ref, wq_ref, wk_ref, wv_ref, q_ref, kv_ref, all_ref, slot_ref, meta_ref,
               cnt, xs, wqb, wkvb, cs, cr, xsnd, xrcv, fs, fr, bs, br, ks, kr, ws):
    t = x_ref.shape[0]
    step = t // PIECES
    loads = [pltpu.make_async_copy(wk_ref, wkvb.at[:, :D], ws.at[0]), pltpu.make_async_copy(wv_ref, wkvb.at[:, D:], ws.at[1]),
             pltpu.make_async_copy(wq_ref, wqb, ws.at[2])]
    for ld in loads:
        ld.start()
    greet(range(1, ne))
    rows = lambda p: pl.ds(p * step, step)
    across = [remote(x_ref.at[rows(p)], xs.at[1, rows(p)], xsnd.at[p], xrcv.at[p], device(2)) for p in range(PIECES)]
    for a in across:
        a.start()
    beside = remote(x_ref, xs.at[0], bs.at[0], br.at[0], device(1))
    beside.start()
    onward = [remote(xs.at[1, rows(p)], xs.at[2, rows(p)], fs.at[p], fr.at[p], device(1)) for p in range(PIECES)]
    lane = lax.broadcasted_iota(jnp.int32, (t, 128), 1)
    named = [idx_ref[:, i:i + 1] == lane for i in range(2)]
    hit = (named[0] | named[1]).astype(jnp.float32)
    before = (lax.broadcasted_iota(jnp.int32, (t, t), 1) < lax.broadcasted_iota(jnp.int32, (t, t), 0)).astype(jnp.bfloat16)
    rank = jnp.dot(before, hit.astype(jnp.bfloat16), preferred_element_type=jnp.float32)
    slot_ref[...] = jnp.transpose(jnp.where(hit > 0, rank, -1.0))[:ne].astype(jnp.int32)
    cnt[...] = jnp.broadcast_to(jnp.sum(hit, axis=0, keepdims=True), (8, 128)).astype(jnp.int32)
    me = lax.axis_index('cp') * (ne // cp) + lax.axis_index('tp')
    place = jnp.bitwise_xor(lane, me).astype(jnp.float32) * (2 * t // ne) + rank
    meta = jnp.zeros((t, 128), jnp.float32)
    for i in range(2):
        at = jnp.sum(jnp.where(named[i], place, 0.0), axis=1, keepdims=True)
        meta = jnp.where(lane == i, at, jnp.where(lane == 2 + i, gate_ref[:, i:i + 1], meta))
    meta_ref[...] = meta
    all_ref[0] = cnt[...]
    counts = [remote(cnt, all_ref.at[r], cs.at[r], cr.at[r], device(r)) for r in range(1, ne)]
    for ld in loads:
        ld.wait()
    sent = []

    def project(block, r, off, n):
        tt = mate(r)
        base = pl.multiple_of(segment(tt, cp) * (2 * t) + lax.rem(tt, 2) * t + off, 16)
        kv_ref[pl.ds(base, n), :] = jnp.dot(block, wkvb[...], preferred_element_type=jnp.float32).astype(jnp.bfloat16)
        qb = pl.multiple_of(tt * t + off, 16)
        q_ref[pl.ds(qb, n), :] = jnp.dot(block, wqb[...], preferred_element_type=jnp.float32).astype(jnp.bfloat16)
        i = len(sent)
        out = remote(kv_ref.at[pl.ds(base, n)], kv_ref.at[pl.ds(base, n)], ks.at[i], kr.at[i], device(4))
        out.start()
        sent.append(out)

    project(x_ref[...], 0, 0, t)
    for cc in counts:
        cc.start()
    beside.wait_recv()
    project(xs[0], 1, 0, t)
    for p in range(PIECES):
        across[p].wait_recv()
        onward[p].start()
        project(xs[1, p * step:(p + 1) * step], 2, p * step, step)
        onward[p].wait_recv()
        project(xs[2, p * step:(p + 1) * step], 3, p * step, step)
    for o in sent:
        o.wait_recv()
    for cc in counts:
        cc.wait_recv()
    for o in counts + across + [beside] + onward + sent:
        o.wait_send()


def qkv(x, idx, gates, wq, wk, wv, cp, ne, cid):
    t, hd = x.shape
    tp = ne // cp
    vm = pl.BlockSpec(memory_space=pltpu.VMEM)
    hb = pl.BlockSpec(memory_space=pl.ANY)
    bf = jnp.bfloat16
    dma = pltpu.SemaphoreType.DMA
    nk = 2 + 2 * PIECES
    return pl.pallas_call(
        functools.partial(qkv_kernel, cp, ne),
        in_specs=[vm, vm, vm, hb, hb, hb], out_specs=[vm] * 5,
        out_shape=[jax.ShapeDtypeStruct((tp * t, wq.shape[1]), bf), jax.ShapeDtypeStruct((ne * t, 2 * D), bf), jax.ShapeDtypeStruct((ne, 8, 128), jnp.int32), jax.ShapeDtypeStruct((ne, t), jnp.int32), jax.ShapeDtypeStruct((t, 128), jnp.float32)],
        scratch_shapes=[pltpu.VMEM((8, 128), jnp.int32), pltpu.VMEM((3, t, hd), bf), pltpu.VMEM(wq.shape, bf), pltpu.VMEM((hd, 2 * D), bf),
                        dma((ne,)), dma((ne,)), dma((PIECES,)), dma((PIECES,)), dma((PIECES,)), dma((PIECES,)), dma((1,)), dma((1,)), dma((nk,)), dma((nk,)), dma((3,))],
        compiler_params=pltpu.CompilerParams(collective_id=cid, has_side_effects=True, vmem_limit_bytes=60 * 1024 * 1024),
        name='qkv')(x, idx, gates, wq, wk, wv)


def attn_kernel(cp, q_ref, kv_ref, x_ref, wo_ref, h_ref, wof, ocat, obuf, m_ref, l_ref, acc_ref, part,
                xs_, xr_, ys_, yr_, ds_, dr_, os_, or_, ls_):
    t, hd = x_ref.shape
    w = wo_ref.shape[0]
    heads = w // D
    half = w // 2
    step = half // CHUNKS
    c = lax.axis_index('cp')
    mine = pltpu.make_async_copy(wo_ref, wof.at[:w], ls_.at[0])
    mine.start()
    greet((1, 2, 3, 4))
    at = lambda base, j: pl.ds(pl.multiple_of(base + j * step, 16), step)
    first, second = c * half, (1 - c) * half
    xc = [remote(wo_ref.at[at(first, j)], wof.at[at(2 * w + first, j)], xs_.at[j], xr_.at[j], device(2)) for j in range(CHUNKS)]
    yc = [remote(wof.at[at(2 * w + first, j)], wof.at[at(2 * w + first, j)], ys_.at[j], yr_.at[j], device(4)) for j in range(CHUNKS)]
    dx = [remote(wof.at[at(2 * w + first, j)], wof.at[at(3 * w + first, j)], ds_.at[j], dr_.at[j], device(1)) for j in range(CHUNKS)]
    dy = [remote(wof.at[at(2 * w + second, j)], wof.at[at(3 * w + second, j)], ds_.at[CHUNKS + j], dr_.at[CHUNKS + j], device(1)) for j in range(CHUNKS)]
    whole = remote(wo_ref, wof.at[pl.ds(w, w)], ds_.at[2 * CHUNKS], dr_.at[2 * CHUNKS], device(1))
    for cpy in xc:
        cpy.start()
    whole.start()

    def relay_x(j):
        xc[j].wait_recv()
        yc[j].start()
        dx[j].start()

    def relay_y(j):
        yc[j].wait_recv()
        dy[j].start()

    scale = D ** -0.5 * math.log2(math.e)
    mask = lax.broadcasted_iota(jnp.int32, (t, t), 1) <= lax.broadcasted_iota(jnp.int32, (t, t), 0)

    def lanes(p):
        s = p[:, :128]
        for a in range(128, t, 128):
            s = s + p[:, a:a + 128]
        return s

    def which(b):
        return jnp.where(b < 2, b + 2, 3 - b)

    def give(b):
        r = which(b)
        return remote(obuf.at[r], ocat.at[:, pl.ds(pl.multiple_of(r * w, 128), w)], os_.at[r], or_.at[r], (lax.axis_index('dp'), c, mate(r)))

    def block(b, u):
        r = which(b)
        tt = mate(r)
        qb = pl.multiple_of(tt * t, t)
        nfull = segment(tt, cp) * 2 + lax.rem(tt, 2)

        def scores(h, j):
            k = kv_ref[pl.ds(pl.multiple_of(j * t, t), t), :D]
            q = q_ref[pl.ds(qb, t), h * D:(h + 1) * D]
            return lax.dot_general(q, k, (((1,), (1,)), ((), ())), preferred_element_type=jnp.float32) * scale

        def pv(p, j):
            v = kv_ref[pl.ds(pl.multiple_of(j * t, t), t), D:]
            return jnp.dot(p.astype(jnp.bfloat16), v, preferred_element_type=jnp.float32)

        for h in range(heads):
            s = jnp.where(mask, scores(h, nfull), -1e30)
            m = jnp.max(s, axis=1, keepdims=True)
            p = jnp.where(mask, jnp.exp2(s - m), 0.0)
            m_ref[h] = jnp.broadcast_to(m, (t, 128))
            l_ref[h] = lanes(p)
            acc_ref[h] = pv(p, nfull)

        @pl.when(b > 0)
        def _():
            give(b - 1).start()

        def body(j, _):
            for n, at_unit in enumerate(HOOKS):
                @pl.when(u + j == at_unit)
                def _():
                    relay_x(n)
            for h in range(heads):
                s = scores(h, j)
                mo = m_ref[h]
                mn = jnp.maximum(mo, jnp.max(s, axis=1, keepdims=True))
                p = jnp.exp2(s - jnp.concatenate([mn] * (t // 128), axis=1))
                al = jnp.exp2(mo - mn)
                m_ref[h] = mn
                l_ref[h] = l_ref[h] * al + lanes(p)
                acc_ref[h] = acc_ref[h] * al + pv(p, j)
            return 0

        lax.fori_loop(0, nfull, body, 0)
        for h in range(heads):
            l = jnp.sum(l_ref[h], axis=1, keepdims=True)
            obuf[r, :, h * D:(h + 1) * D] = (acc_ref[h] / l).astype(jnp.bfloat16)
        return u + nfull

    units = lax.fori_loop(0, 4, block, 0)
    ocat[:, :w] = obuf[0]
    mine.wait()
    whole.wait_recv()
    give(2).wait_recv()

    def near(n, _):
        cols = pl.ds(pl.multiple_of(n * NT, NT), NT)
        part[:, cols] = jnp.dot(ocat[:, :2 * w], wof[:2 * w, cols], preferred_element_type=jnp.float32)
        return 0
    lax.fori_loop(0, hd // NT, near, 0)
    relay_x(2)
    relay_y(0)
    relay_x(3)
    relay_y(1)
    relay_y(2)
    relay_y(3)
    for j in range(CHUNKS):
        dx[j].wait_recv()
        dy[j].wait_recv()
    give(0).wait_recv()
    give(1).wait_recv()

    def far(n, _):
        cols = pl.ds(pl.multiple_of(n * NT, NT), NT)
        s = part[:, cols] + jnp.dot(ocat[:, 2 * w:], wof[2 * w:, cols], preferred_element_type=jnp.float32)
        h_ref[:, cols] = (x_ref[:, cols].astype(jnp.float32) + s).astype(jnp.bfloat16)
        return 0
    lax.fori_loop(0, hd // NT, far, 0)
    for cpy in xc + yc + dx + dy + [whole, give(0), give(1), give(2)]:
        cpy.wait_send()


def attention(q, kv, x, wo, cp, cid):
    t, hd = x.shape
    w = wo.shape[0]
    heads = w // D
    vm = pl.BlockSpec(memory_space=pltpu.VMEM)
    hb = pl.BlockSpec(memory_space=pl.ANY)
    bf = jnp.bfloat16
    dma = pltpu.SemaphoreType.DMA
    state = pltpu.VMEM((heads, t, 128), jnp.float32)
    return pl.pallas_call(
        functools.partial(attn_kernel, cp),
        in_specs=[vm, vm, vm, hb], out_specs=vm,
        out_shape=jax.ShapeDtypeStruct((t, hd), bf),
        scratch_shapes=[pltpu.VMEM((4 * w, hd), bf), pltpu.VMEM((t, 4 * w), bf), pltpu.VMEM((4, t, w), bf), state, state, state, pltpu.VMEM((t, hd), jnp.float32),
                        dma((CHUNKS,)), dma((CHUNKS,)), dma((CHUNKS,)), dma((CHUNKS,)), dma((2 * CHUNKS + 1,)), dma((2 * CHUNKS + 1,)), dma((4,)), dma((4,)), dma((1,))],
        compiler_params=pltpu.CompilerParams(collective_id=cid, has_side_effects=True, vmem_limit_bytes=63 * 1024 * 1024),
        name='attn')(q, kv, x, wo)


def expert_ffn(rows, wg, wu, wd):
    gg = jnp.dot(rows, wg, preferred_element_type=jnp.float32)
    uu = jnp.dot(rows, wu, preferred_element_type=jnp.float32)
    act = (jax.nn.silu(gg) * uu).astype(jnp.bfloat16)
    return jnp.dot(act, wd, preferred_element_type=jnp.float32).astype(jnp.bfloat16)


def moe_any(h, slot, idx, gates, wg, wu, wd):
    t, hd = h.shape
    ne = slot.shape[0]
    cap = 4 * t // ne
    pick = (slot[:, None, :] == jnp.arange(cap)[None, :, None]).astype(jnp.bfloat16).reshape(ne * cap, t)
    send = jnp.dot(pick, h, preferred_element_type=jnp.float32).astype(jnp.bfloat16)
    recv = lax.all_to_all(send.reshape(ne, cap, hd), ('cp', 'tp'), 0, 0, tiled=True)
    z = expert_ffn(recv.reshape(ne * cap, hd), wg, wu, wd)
    back = lax.all_to_all(z.reshape(ne, cap, hd), ('cp', 'tp'), 0, 0, tiled=True).reshape(ne * cap, hd)
    flat = jnp.arange(ne * cap)
    y = h.astype(jnp.float32)
    for k in range(2):
        mine = jnp.sum(jnp.where(idx[:, k][None, :] == jnp.arange(ne)[:, None], jnp.arange(ne)[:, None] * cap + slot, 0), axis=0)
        sel = (mine[:, None] == flat[None, :]).astype(jnp.bfloat16)
        y = y + gates[:, k:k + 1] * jnp.dot(sel, back, preferred_element_type=jnp.float32)
    return y.astype(jnp.bfloat16)


def solution(mesh):
    cp = mesh.shape['cp']
    tp = mesh.shape['tp']
    ne = cp * tp
    rows_spec = P(('dp', 'cp', 'tp'), None)
    exp_spec = P(('cp', 'tp'), None, None)

    def local(x, idx, gates, wq, wk, wv, wo, w1g, w1u, w2):
        t, hd = x.shape
        q, kv, counts, slot, meta = qkv(x, idx, gates, wq, wk, wv, cp, ne, 1)
        h = attention(q, kv, x, wo, cp, 2)
        worst = jnp.max(counts)

        def tight(h):
            return moe_fast(h, slot, meta, w1g[0], w1u[0], w2[0], t // 4, 3)

        def roomy(h):
            return moe_any(h, slot, idx, gates, w1g[0], w1u[0], w2[0])

        return lax.cond(worst <= t // 4, tight, roomy, h)

    return jax.shard_map(local, mesh=mesh, in_specs=(rows_spec, rows_spec, rows_spec, P(None, 'tp'), P(None, 'tp'), P(None, 'tp'), P('tp', None), exp_spec, exp_spec, exp_spec), out_specs=rows_spec, check_vma=False)
```

```python
import functools
import math

import jax
import jax.numpy as jnp
from jax import lax
from jax.experimental import pallas as pl
from jax.experimental.pallas import tpu as pltpu
from jax.sharding import PartitionSpec as P


MESH = pl.DeviceIdType.MESH
NEAR = 6
FT = 512
NT = 512


def peer(r):
    c, t = lax.axis_index('cp'), lax.axis_index('tp')
    core, xx = lax.rem(t, 2), t // 2
    core = 1 - core if r & 1 else core
    xx = 1 - xx if r & 2 else xx
    c = 1 - c if r & 4 else c
    return c, xx * 2 + core


def device(r):
    c, t = peer(r)
    return (lax.axis_index('dp'), c, t)


def hail(peers):
    bar = pltpu.get_barrier_semaphore()
    for r in peers:
        pl.semaphore_signal(bar, inc=1, device_id=device(r), device_id_type=MESH)


def greet(peers):
    hail(peers)
    pl.semaphore_wait(pltpu.get_barrier_semaphore(), len(peers))


def moe_kernel(ne, cap, h_ref, slot_ref, meta_ref, w1g_ref, w1u_ref, w2_ref, y_ref,
               send, recv, act, zsend, zrecv, sel, pick, w1b, w2b, ds, dr, zs, zr, zf, w1s, w2s):
    t, hd = h_ref.shape
    ff = w2_ref.shape[0]
    nf, nz = ff // FT, hd // NT

    def w1_copy(tile, slot, which):
        src = (w1g_ref, w1u_ref)[which]
        return pltpu.make_async_copy(src.at[:, pl.ds(pl.multiple_of(tile * FT, FT), FT)], w1b.at[slot, which], w1s.at[slot, which])

    def w2_copy(tile, slot):
        return pltpu.make_async_copy(w2_ref.at[:, pl.ds(pl.multiple_of(tile * NT, NT), NT)], w2b.at[slot], w2s.at[slot])

    for s in range(2):
        w1_copy(s, s, 0).start()
        w1_copy(s, s, 1).start()
    for s in range(2):
        w2_copy(s, s).start()

    hail(range(1, ne))
    tile = lambda n: pl.ds(pl.multiple_of(n * NT, NT), NT)

    def out_copy(r, cols=slice(None)):
        return pltpu.make_async_remote_copy(src_ref=send.at[r, :, cols], dst_ref=recv.at[r, :, cols], send_sem=ds.at[r], recv_sem=dr.at[r], device_id=device(r), device_id_type=MESH)

    for r in range(ne):
        c, tt = peer(r)
        row = slot_ref[pl.ds(c * (ne // 2) + tt, 1), :]
        sel[r * cap:(r + 1) * cap, :] = (jnp.broadcast_to(row, (cap, t)) == lax.broadcasted_iota(jnp.int32, (cap, t), 0)).astype(jnp.bfloat16)
    pl.semaphore_wait(pltpu.get_barrier_semaphore(), ne - 1)

    def dispatch(lo, hi, order):
        def one(n, _):
            rows = jnp.dot(sel[lo * cap:hi * cap, :], h_ref[:, tile(n)], preferred_element_type=jnp.float32).astype(jnp.bfloat16)
            for r in range(lo, hi):
                dst = recv if r == 0 else send
                dst[r, :, tile(n)] = rows[(r - lo) * cap:(r - lo + 1) * cap]

            @pl.when(n > 0)
            def _():
                for r in order:
                    out_copy(r, tile(n - 1)).start()
            return 0
        lax.fori_loop(0, nz, one, 0)
        for r in order:
            out_copy(r, tile(nz - 1)).start()

    dispatch(0, NEAR, (2, 4, 3, 5, 1))
    dispatch(NEAR, ne, (6, 7))
    for k in range(2):
        pick[k * t:(k + 1) * t, :] = (meta_ref[:, k:k + 1] == lax.broadcasted_iota(jnp.int32, (t, ne * cap), 1).astype(jnp.float32)).astype(jnp.bfloat16)

    def back_copy(r, n):
        got = zr.at[r] if r < NEAR else zf.at[r - NEAR, n]
        return pltpu.make_async_remote_copy(src_ref=zsend.at[r, :, tile(n)], dst_ref=zrecv.at[r, :, tile(n)], send_sem=zs.at[r], recv_sem=got, device_id=device(r), device_id_type=MESH)

    def experts(lo, hi, again):
        rows = (hi - lo) * cap
        off, off1 = (0, 0) if again else (nz, nf)

        def up(f, _):
            slot = lax.rem(f + off1, 2)
            w1_copy(f, slot, 0).wait()
            w1_copy(f, slot, 1).wait()
            xr = recv[lo:hi].reshape(rows, hd)
            gg = jnp.dot(xr, w1b[slot, 0], preferred_element_type=jnp.float32)
            uu = jnp.dot(xr, w1b[slot, 1], preferred_element_type=jnp.float32)
            act[:rows, pl.ds(pl.multiple_of(f * FT, FT), FT)] = (gg * jax.nn.sigmoid(gg) * uu).astype(jnp.bfloat16)
            nxt = f + 2

            @pl.when(nxt < (nf + 2 if again else nf))
            def _():
                w1_copy(lax.rem(nxt, nf), slot, 0).start()
                w1_copy(lax.rem(nxt, nf), slot, 1).start()
            return 0
        lax.fori_loop(0, nf, up, 0)

        def down(n, _):
            slot = lax.rem(n + off, 2)
            w2_copy(n, slot).wait()

            @pl.when(n > 0)
            def _():
                for r in range(max(lo, 1), hi):
                    back_copy(r, n - 1).start()
            zz = jnp.dot(act[:rows], w2b[slot], preferred_element_type=jnp.float32).astype(jnp.bfloat16)
            cols = pl.ds(pl.multiple_of(n * NT, NT), NT)
            for r in range(lo, hi):
                dst = zrecv if r == 0 else zsend
                dst[r, :, cols] = zz[(r - lo) * cap:(r - lo + 1) * cap]
            nxt = n + 2

            @pl.when(nxt < (nz + 2 if again else nz))
            def _():
                w2_copy(lax.rem(nxt, nz), slot).start()
            return 0
        lax.fori_loop(0, nz, down, 0)
        for r in range(max(lo, 1), hi):
            back_copy(r, nz - 1).start()

    for r in range(1, NEAR):
        out_copy(r).wait_recv()
    experts(0, NEAR, True)
    for r in range(NEAR, ne):
        out_copy(r).wait_recv()
    experts(NEAR, ne, False)
    whole = lambda r: pltpu.make_async_remote_copy(src_ref=zsend.at[r], dst_ref=zrecv.at[r], send_sem=zs.at[r], recv_sem=zr.at[r], device_id=device(r), device_id_type=MESH)
    for r in range(1, NEAR):
        whole(r).wait_recv()

    def combine(n, _):
        cols = tile(n)
        for r in range(NEAR, ne):
            back_copy(r, n).wait_recv()
        zt = jnp.dot(pick[...], zrecv[:, :, cols].reshape(ne * cap, NT), preferred_element_type=jnp.float32)
        y = h_ref[:, cols].astype(jnp.float32) + (meta_ref[:, 2:3] * zt[:t] + meta_ref[:, 3:4] * zt[t:])
        y_ref[:, cols] = y.astype(jnp.bfloat16)
        return 0
    lax.fori_loop(0, nz, combine, 0)
    for r in range(1, ne):
        out_copy(r).wait_send()
        whole(r).wait_send()


def moe_fast(h, slot, meta, w1g, w1u, w2, cap, cid):
    t, hd = h.shape
    ne = slot.shape[0]
    vm = pl.BlockSpec(memory_space=pltpu.VMEM)
    hb = pl.BlockSpec(memory_space=pl.ANY)
    bf = jnp.bfloat16
    ff = w2.shape[0]
    return pl.pallas_call(
        functools.partial(moe_kernel, ne, cap),
        in_specs=[vm, vm, vm, hb, hb, hb], out_specs=vm,
        out_shape=jax.ShapeDtypeStruct((t, hd), bf),
        scratch_shapes=[pltpu.VMEM((ne, cap, hd), bf), pltpu.VMEM((ne, cap, hd), bf), pltpu.VMEM((NEAR * cap, ff), bf),
                        pltpu.VMEM((ne, cap, hd), bf), pltpu.VMEM((ne, cap, hd), bf), pltpu.VMEM((ne * cap, t), bf), pltpu.VMEM((2 * t, ne * cap), bf),
                        pltpu.VMEM((2, 2, hd, FT), bf), pltpu.VMEM((2, ff, NT), bf)]
                       + [pltpu.SemaphoreType.DMA((ne,))] * 4 + [pltpu.SemaphoreType.DMA((ne - NEAR, hd // NT))] + [pltpu.SemaphoreType.DMA((2, 2)), pltpu.SemaphoreType.DMA((2,))],
        compiler_params=pltpu.CompilerParams(collective_id=cid, has_side_effects=True, vmem_limit_bytes=63 * 1024 * 1024),
        name='moe')(h, slot, meta, w1g, w1u, w2)


D = 128
PIECES = 4
CHUNKS = 4
HOOKS = (2, 8, 13)


def mate(r):
    t = lax.axis_index('tp')
    core = lax.rem(lax.rem(t, 2) + lax.rem(r, 2), 2)
    xx = lax.rem(t // 2 + r // 2, 2)
    return xx * 2 + core


def segment(t, cp):
    c = lax.axis_index('cp')
    return jnp.where(t < 2, c, 2 * cp - 1 - c)


def remote(src, dst, send, recv, dev):
    return pltpu.make_async_remote_copy(src_ref=src, dst_ref=dst, send_sem=send, recv_sem=recv, device_id=dev, device_id_type=MESH)


def route(ne, cp, idx_ref, gate_ref, slot_ref, meta_ref, cnt):
    t = idx_ref.shape[1]
    lab = lax.broadcasted_iota(jnp.int32, (128, t), 0)
    named = [idx_ref[i:i + 1, :] == lab for i in range(2)]
    hit = (named[0] | named[1]).astype(jnp.float32)
    before = (lax.broadcasted_iota(jnp.int32, (t, t), 0) < lax.broadcasted_iota(jnp.int32, (t, t), 1)).astype(jnp.bfloat16)
    rank = jnp.dot(hit.astype(jnp.bfloat16), before, preferred_element_type=jnp.float32)
    slot_ref[...] = jnp.where(hit > 0, rank, -1.0)[:ne].astype(jnp.int32)
    cnt[...] = jnp.broadcast_to(jnp.sum(hit[:8], axis=1, keepdims=True), (8, 128)).astype(jnp.int32)
    me = lax.axis_index('cp') * (ne // cp) + lax.axis_index('tp')
    place = jnp.bitwise_xor(lab, me).astype(jnp.float32) * (2 * t // ne) + rank
    meta = jnp.zeros((128, t), jnp.float32)
    for i in range(2):
        at = jnp.sum(jnp.where(named[i], place, 0.0), axis=0, keepdims=True)
        meta = jnp.where(lab == i, at, jnp.where(lab == 2 + i, gate_ref[i:i + 1, :], meta))
    meta_ref[...] = jnp.transpose(meta)


def front_kernel(cp, ne, x_ref, idx_ref, gate_ref, wq_ref, wk_ref, wv_ref, wo_ref, h_ref, all_ref, slot_ref, meta_ref,
                 cnt, xs, wqb, wkvb, q_ref, kv_ref, wof, ocat, st,
                 cs, cr, as_, ar_, fs, fr, bs, br, ks, kr, ws, xs_, xr_, ys_, yr_, ds_, dr_, os_, or_, ls_, hs_):
    t, hd = x_ref.shape
    c = lax.axis_index('cp')
    loads = [pltpu.make_async_copy(wk_ref, wkvb.at[:, :D], ws.at[0]), pltpu.make_async_copy(wv_ref, wkvb.at[:, D:], ws.at[1]),
             pltpu.make_async_copy(wq_ref, wqb, ws.at[2])]
    for ld in loads:
        ld.start()
    greet(range(1, ne))

    step = t // PIECES
    rows = lambda p: pl.ds(pl.multiple_of(p * step, 16), step)
    across = lambda p: remote(x_ref.at[rows(p)], xs.at[1, rows(p)], as_.at[p], ar_.at[p], device(2))
    onward = lambda p: remote(xs.at[1, rows(p)], xs.at[2, rows(p)], fs.at[p], fr.at[p], device(1))
    beside = remote(x_ref, xs.at[0], bs.at[0], br.at[0], device(1))
    for p in range(2):
        across(p).start()
    beside.start()
    route(ne, cp, idx_ref, gate_ref, slot_ref, meta_ref, cnt)
    all_ref[0] = cnt[...]
    counts = [remote(cnt, all_ref.at[r], cs.at[r], cr.at[r], device(r)) for r in range(1, ne)]

    w = wo_ref.shape[0]
    heads = w // D
    half = w // 2
    cut = half // CHUNKS
    at = lambda base, j: pl.ds(pl.multiple_of(base + j * cut, 16), cut)
    first, second = c * half, (1 - c) * half
    mine = pltpu.make_async_copy(wo_ref, wof.at[:w], ls_.at[0])
    xc = [remote(wo_ref.at[at(first, j)], wof.at[at(2 * w + first, j)], xs_.at[j], xr_.at[j], device(2)) for j in range(CHUNKS)]
    yc = [remote(wof.at[at(2 * w + first, j)], wof.at[at(2 * w + first, j)], ys_.at[j], yr_.at[j], device(4)) for j in range(CHUNKS)]
    dx = [remote(wof.at[at(2 * w + first, j)], wof.at[at(3 * w + first, j)], ds_.at[j], dr_.at[j], device(1)) for j in range(CHUNKS)]
    dy = [remote(wof.at[at(2 * w + second, j)], wof.at[at(3 * w + second, j)], ds_.at[CHUNKS + j], dr_.at[CHUNKS + j], device(1)) for j in range(CHUNKS)]
    whole = remote(wo_ref, wof.at[pl.ds(w, w)], ds_.at[2 * CHUNKS], dr_.at[2 * CHUNKS], device(1))

    def relay_x(j):
        xc[j].wait_recv()
        yc[j].start()
        dx[j].start()

    def relay_y(j):
        yc[j].wait_recv()
        dy[j].start()

    def pair(i, base, n):
        return remote(kv_ref.at[pl.ds(base, n)], kv_ref.at[pl.ds(base, n)], ks.at[i], kr.at[i], device(4))

    def project(block, r, off, n, i):
        tt = mate(r)
        base = pl.multiple_of(segment(tt, cp) * (2 * t) + lax.rem(tt, 2) * t + off, 16)
        kv_ref[pl.ds(base, n), :] = jnp.dot(block, wkvb[...], preferred_element_type=jnp.float32).astype(jnp.bfloat16)
        qb = pl.multiple_of(tt * t + off, 16)
        q_ref[pl.ds(qb, n), :] = jnp.dot(block, wqb[...], preferred_element_type=jnp.float32).astype(jnp.bfloat16)
        pair(i, base, n).start()

    for cc in counts:
        cc.start()
    for p in range(2, PIECES):
        across(p).start()
    for ld in loads:
        ld.wait()
    project(x_ref[...], 0, 0, t, 0)
    beside.wait_recv()
    project(xs[0], 1, 0, t, 1)

    def land(p, _):
        across(p).wait_recv()
        onward(p).start()

        @pl.when(p == 2)
        def _():
            for cpy in xc:
                cpy.start()
        project(xs[1, rows(p)], 2, p * step, step, 2 + 2 * p)
        onward(p).wait_recv()
        project(xs[2, rows(p)], 3, p * step, step, 3 + 2 * p)
        return 0
    lax.fori_loop(0, PIECES, land, 0)
    mine.start()
    whole.start()
    for i in range(2):
        pair(i, 0, t).wait_recv()
    for i in range(2, 2 + 2 * PIECES):
        pair(i, 0, step).wait_recv()
    for p in range(PIECES):
        onward(p).wait_send()

    scale = D ** -0.5 * math.log2(math.e)
    mask = lax.broadcasted_iota(jnp.int32, (t, t), 1) <= lax.broadcasted_iota(jnp.int32, (t, t), 0)
    M, L, A = 0, heads, 2 * heads

    def lanes(p):
        s = p[:, :128]
        for a in range(128, t, 128):
            s = s + p[:, a:a + 128]
        return s

    def which(b):
        return jnp.where(b < 2, b + 2, 3 - b)

    def give(b):
        r = which(b)
        cols = pl.ds(pl.multiple_of(r * w, 128), w)
        return remote(xs.at[2, :, cols], ocat.at[:, cols], os_.at[r], or_.at[r], (lax.axis_index('dp'), c, mate(r)))

    def block(b, u):
        r = which(b)
        tt = mate(r)
        qb = pl.multiple_of(tt * t, t)
        nfull = segment(tt, cp) * 2 + lax.rem(tt, 2)

        def scores(h, j):
            k = kv_ref[pl.ds(pl.multiple_of(j * t, t), t), :D]
            q = q_ref[pl.ds(qb, t), h * D:(h + 1) * D]
            return lax.dot_general(q, k, (((1,), (1,)), ((), ())), preferred_element_type=jnp.float32) * scale

        def pv(p, j):
            v = kv_ref[pl.ds(pl.multiple_of(j * t, t), t), D:]
            return jnp.dot(p.astype(jnp.bfloat16), v, preferred_element_type=jnp.float32)

        for h in range(heads):
            s = jnp.where(mask, scores(h, nfull), -1e30)
            m = jnp.max(s, axis=1, keepdims=True)
            p = jnp.where(mask, jnp.exp2(s - m), 0.0)
            st[M + h] = jnp.broadcast_to(m, (t, 128))
            st[L + h] = lanes(p)
            st[A + h] = pv(p, nfull)

        @pl.when(b > 0)
        def _():
            give(b - 1).start()

        def body(j, _):
            for n, at_unit in enumerate(HOOKS):
                @pl.when(u + j == at_unit)
                def _():
                    relay_x(n)
            for h in range(heads):
                s = scores(h, j)
                mo = st[M + h]
                mn = jnp.maximum(mo, jnp.max(s, axis=1, keepdims=True))
                p = jnp.exp2(s - jnp.concatenate([mn] * (t // 128), axis=1))
                al = jnp.exp2(mo - mn)
                st[M + h] = mn
                st[L + h] = st[L + h] * al + lanes(p)
                st[A + h] = st[A + h] * al + pv(p, j)
            return 0

        lax.fori_loop(0, nfull, body, 0)
        for h in range(heads):
            l = jnp.sum(st[L + h], axis=1, keepdims=True)
            xs[2, :, pl.ds(pl.multiple_of(r * w + h * D, 128), D)] = (st[A + h] / l).astype(jnp.bfloat16)
        return u + nfull

    lax.fori_loop(0, 4, block, 0)
    ocat[:, :w] = xs[2, :, :w]

    tile = lambda n: pl.ds(pl.multiple_of(n * NT, NT), NT)
    per = NT // 128

    def held(n):
        return jnp.concatenate([st[n * per + i] for i in range(per)], axis=1)

    def add(lo, hi, fresh):
        def one(n, _):
            s = jnp.dot(ocat[:, lo * w:hi * w], wof[lo * w:hi * w, tile(n)], preferred_element_type=jnp.float32)
            if not fresh:
                s = s + held(n)
            for i in range(per):
                st[n * per + i] = s[:, i * 128:(i + 1) * 128]
            return 0
        lax.fori_loop(0, hd // NT, one, 0)

    mine.wait()
    whole.wait_recv()
    give(2).wait_recv()
    add(0, 2, True)
    relay_y(0)
    for j in range(len(HOOKS), CHUNKS):
        relay_x(j)
    for j in range(1, CHUNKS):
        relay_y(j)
    for j in range(CHUNKS):
        dx[j].wait_recv()
        dy[j].wait_recv()
    give(0).wait_recv()
    add(2, 3, False)
    give(1).wait_recv()
    out = lambda n: pltpu.make_async_copy(xs.at[0, :, tile(n)], h_ref.at[:, tile(n)], hs_.at[0])

    def last(n, _):
        s = held(n) + jnp.dot(ocat[:, 3 * w:], wof[3 * w:, tile(n)], preferred_element_type=jnp.float32)
        xs[0, :, tile(n)] = (x_ref[:, tile(n)].astype(jnp.float32) + s).astype(jnp.bfloat16)

        @pl.when(n > 0)
        def _():
            out(n - 1).start()
        return 0
    lax.fori_loop(0, hd // NT, last, 0)
    out(hd // NT - 1).start()
    for cc in counts:
        cc.wait_recv()
    for p in range(PIECES):
        across(p).wait_send()
    for i in range(2):
        pair(i, 0, t).wait_send()
    for i in range(2, 2 + 2 * PIECES):
        pair(i, 0, step).wait_send()
    for cpy in counts + [beside] + xc + yc + dx + dy + [whole, give(0), give(1), give(2)]:
        cpy.wait_send()
    pltpu.make_async_copy(xs.at[0], h_ref, hs_.at[0]).wait()


def front(x, idx, gates, wq, wk, wv, wo, cp, ne, cid):
    t, hd = x.shape
    tp = ne // cp
    w = wo.shape[0]
    vm = pl.BlockSpec(memory_space=pltpu.VMEM)
    hb = pl.BlockSpec(memory_space=pl.ANY)
    bf = jnp.bfloat16
    dma = lambda n: pltpu.SemaphoreType.DMA((n,))
    nk = 2 + 2 * PIECES
    nd = 2 * CHUNKS + 1
    return pl.pallas_call(
        functools.partial(front_kernel, cp, ne),
        in_specs=[vm, vm, vm, hb, hb, hb, hb], out_specs=[hb, vm, vm, vm],
        out_shape=[jax.ShapeDtypeStruct((t, hd), bf), jax.ShapeDtypeStruct((ne, 8, 128), jnp.int32), jax.ShapeDtypeStruct((ne, t), jnp.int32), jax.ShapeDtypeStruct((t, 128), jnp.float32)],
        scratch_shapes=[pltpu.VMEM((8, 128), jnp.int32), pltpu.VMEM((3, t, hd), bf), pltpu.VMEM(wq.shape, bf), pltpu.VMEM((hd, 2 * D), bf),
                        pltpu.VMEM((tp * t, w), bf), pltpu.VMEM((ne * t, 2 * D), bf), pltpu.VMEM((tp * w, hd), bf), pltpu.VMEM((t, tp * w), bf), pltpu.VMEM((hd // 128, t, 128), jnp.float32),
                        dma(ne), dma(ne), dma(PIECES), dma(PIECES), dma(PIECES), dma(PIECES), dma(1), dma(1), dma(nk), dma(nk), dma(3),
                        dma(CHUNKS), dma(CHUNKS), dma(CHUNKS), dma(CHUNKS), dma(nd), dma(nd), dma(4), dma(4), dma(1), dma(1)],
        compiler_params=pltpu.CompilerParams(collective_id=cid, has_side_effects=True, vmem_limit_bytes=67043328),
        name='front')(x, idx.T, gates.T, wq, wk, wv, wo)


def expert_ffn(rows, wg, wu, wd):
    gg = jnp.dot(rows, wg, preferred_element_type=jnp.float32)
    uu = jnp.dot(rows, wu, preferred_element_type=jnp.float32)
    act = (jax.nn.silu(gg) * uu).astype(jnp.bfloat16)
    return jnp.dot(act, wd, preferred_element_type=jnp.float32).astype(jnp.bfloat16)


def moe_any(h, slot, idx, gates, wg, wu, wd):
    t, hd = h.shape
    ne = slot.shape[0]
    cap = 4 * t // ne
    pick = (slot[:, None, :] == jnp.arange(cap)[None, :, None]).astype(jnp.bfloat16).reshape(ne * cap, t)
    send = jnp.dot(pick, h, preferred_element_type=jnp.float32).astype(jnp.bfloat16)
    recv = lax.all_to_all(send.reshape(ne, cap, hd), ('cp', 'tp'), 0, 0, tiled=True)
    z = expert_ffn(recv.reshape(ne * cap, hd), wg, wu, wd)
    back = lax.all_to_all(z.reshape(ne, cap, hd), ('cp', 'tp'), 0, 0, tiled=True).reshape(ne * cap, hd)
    flat = jnp.arange(ne * cap)
    y = h.astype(jnp.float32)
    for k in range(2):
        mine = jnp.sum(jnp.where(idx[:, k][None, :] == jnp.arange(ne)[:, None], jnp.arange(ne)[:, None] * cap + slot, 0), axis=0)
        sel = (mine[:, None] == flat[None, :]).astype(jnp.bfloat16)
        y = y + gates[:, k:k + 1] * jnp.dot(sel, back, preferred_element_type=jnp.float32)
    return y.astype(jnp.bfloat16)


def solution(mesh):
    cp = mesh.shape['cp']
    tp = mesh.shape['tp']
    ne = cp * tp
    rows_spec = P(('dp', 'cp', 'tp'), None)
    exp_spec = P(('cp', 'tp'), None, None)

    def local(x, idx, gates, wq, wk, wv, wo, w1g, w1u, w2):
        t, hd = x.shape
        h, counts, slot, meta = front(x, idx, gates, wq, wk, wv, wo, cp, ne, 1)
        worst = jnp.max(counts)

        def tight(h):
            return moe_fast(h, slot, meta, w1g[0], w1u[0], w2[0], t // 4, 3)

        def roomy(h):
            return moe_any(h, slot, idx, gates, w1g[0], w1u[0], w2[0])

        return lax.cond(worst <= t // 4, tight, roomy, h)

    return jax.shard_map(local, mesh=mesh, in_specs=(rows_spec, rows_spec, rows_spec, P(None, 'tp'), P(None, 'tp'), P(None, 'tp'), P('tp', None), exp_spec, exp_spec, exp_spec), out_specs=rows_spec, check_vma=False)
```

```python
import functools
import math

import jax
import jax.numpy as jnp
from jax import lax
from jax.experimental import pallas as pl
from jax.experimental.pallas import tpu as pltpu
from jax.sharding import PartitionSpec as P


MESH = pl.DeviceIdType.MESH
NEAR = 6
FT = 512
NT = 512


def peer(r):
    c, t = lax.axis_index('cp'), lax.axis_index('tp')
    core, xx = lax.rem(t, 2), t // 2
    core = 1 - core if r & 1 else core
    xx = 1 - xx if r & 2 else xx
    c = 1 - c if r & 4 else c
    return c, xx * 2 + core


def device(r):
    c, t = peer(r)
    return (lax.axis_index('dp'), c, t)


def hail(peers):
    bar = pltpu.get_barrier_semaphore()
    for r in peers:
        pl.semaphore_signal(bar, inc=1, device_id=device(r), device_id_type=MESH)


def greet(peers):
    hail(peers)
    pl.semaphore_wait(pltpu.get_barrier_semaphore(), len(peers))


def moe_kernel(ne, cap, hin_ref, slot_ref, meta_ref, w1g_ref, w1u_ref, w2_ref, yout_ref,
               h_ref, y_ref, send, recv, act, zsend, zrecv, sel, pick, w1b, w2b, ds, dr, zs, zr, zf, w1s, w2s, hs, ys):
    t, hd = h_ref.shape
    hload = pltpu.make_async_copy(hin_ref, h_ref, hs.at[0])
    hload.start()
    hail(range(1, ne))
    ff = w2_ref.shape[0]
    nf, nz = ff // FT, hd // NT

    def w1_copy(tile, slot, which):
        src = (w1g_ref, w1u_ref)[which]
        return pltpu.make_async_copy(src.at[:, pl.ds(pl.multiple_of(tile * FT, FT), FT)], w1b.at[slot, which], w1s.at[slot, which])

    def w2_copy(tile, slot):
        return pltpu.make_async_copy(w2_ref.at[:, pl.ds(pl.multiple_of(tile * NT, NT), NT)], w2b.at[slot], w2s.at[slot])

    for s in range(2):
        w1_copy(s, s, 0).start()
        w1_copy(s, s, 1).start()
    for s in range(2):
        w2_copy(s, s).start()

    tile = lambda n: pl.ds(pl.multiple_of(n * NT, NT), NT)

    def out_copy(r, cols=slice(None)):
        return pltpu.make_async_remote_copy(src_ref=send.at[r, :, cols], dst_ref=recv.at[r, :, cols], send_sem=ds.at[r], recv_sem=dr.at[r], device_id=device(r), device_id_type=MESH)

    for r in range(ne):
        c, tt = peer(r)
        row = slot_ref[pl.ds(c * (ne // 2) + tt, 1), :]
        sel[r * cap:(r + 1) * cap, :] = (jnp.broadcast_to(row, (cap, t)) == lax.broadcasted_iota(jnp.int32, (cap, t), 0)).astype(jnp.bfloat16)
    hload.wait()
    pl.semaphore_wait(pltpu.get_barrier_semaphore(), ne - 1)

    def dispatch(lo, hi, order):
        def one(n, _):
            rows = jnp.dot(sel[lo * cap:hi * cap, :], h_ref[:, tile(n)], preferred_element_type=jnp.float32).astype(jnp.bfloat16)
            for r in range(lo, hi):
                dst = recv if r == 0 else send
                dst[r, :, tile(n)] = rows[(r - lo) * cap:(r - lo + 1) * cap]

            @pl.when(n > 0)
            def _():
                for r in order:
                    out_copy(r, tile(n - 1)).start()
            return 0
        lax.fori_loop(0, nz, one, 0)
        for r in order:
            out_copy(r, tile(nz - 1)).start()

    dispatch(0, NEAR, (2, 4, 3, 5, 1))
    dispatch(NEAR, ne, (6, 7))
    for k in range(2):
        pick[k * t:(k + 1) * t, :] = (meta_ref[:, k:k + 1] == lax.broadcasted_iota(jnp.int32, (t, ne * cap), 1).astype(jnp.float32)).astype(jnp.bfloat16)

    def back_copy(r, n):
        got = zr.at[r] if r < NEAR else zf.at[r - NEAR, n]
        return pltpu.make_async_remote_copy(src_ref=zsend.at[r, :, tile(n)], dst_ref=zrecv.at[r, :, tile(n)], send_sem=zs.at[r], recv_sem=got, device_id=device(r), device_id_type=MESH)

    def experts(lo, hi, again):
        rows = (hi - lo) * cap
        off, off1 = (0, 0) if again else (nz, nf)

        def up(f, _):
            slot = lax.rem(f + off1, 2)
            w1_copy(f, slot, 0).wait()
            w1_copy(f, slot, 1).wait()
            xr = recv[lo:hi].reshape(rows, hd)
            gg = jnp.dot(xr, w1b[slot, 0], preferred_element_type=jnp.float32)
            uu = jnp.dot(xr, w1b[slot, 1], preferred_element_type=jnp.float32)
            act[:rows, pl.ds(pl.multiple_of(f * FT, FT), FT)] = (gg * jax.nn.sigmoid(gg) * uu).astype(jnp.bfloat16)
            nxt = f + 2

            @pl.when(nxt < (nf + 2 if again else nf))
            def _():
                w1_copy(lax.rem(nxt, nf), slot, 0).start()
                w1_copy(lax.rem(nxt, nf), slot, 1).start()
            return 0
        lax.fori_loop(0, nf, up, 0)

        def down(n, _):
            slot = lax.rem(n + off, 2)
            w2_copy(n, slot).wait()

            @pl.when(n > 0)
            def _():
                for r in range(max(lo, 1), hi):
                    back_copy(r, n - 1).start()
            zz = jnp.dot(act[:rows], w2b[slot], preferred_element_type=jnp.float32).astype(jnp.bfloat16)
            cols = pl.ds(pl.multiple_of(n * NT, NT), NT)
            for r in range(lo, hi):
                dst = zrecv if r == 0 else zsend
                dst[r, :, cols] = zz[(r - lo) * cap:(r - lo + 1) * cap]
            nxt = n + 2

            @pl.when(nxt < (nz + 2 if again else nz))
            def _():
                w2_copy(lax.rem(nxt, nz), slot).start()
            return 0
        lax.fori_loop(0, nz, down, 0)
        for r in range(max(lo, 1), hi):
            back_copy(r, nz - 1).start()

    for r in range(1, NEAR):
        out_copy(r).wait_recv()
    experts(0, NEAR, True)
    for r in range(NEAR, ne):
        out_copy(r).wait_recv()
    experts(NEAR, ne, False)
    whole = lambda r: pltpu.make_async_remote_copy(src_ref=zsend.at[r], dst_ref=zrecv.at[r], send_sem=zs.at[r], recv_sem=zr.at[r], device_id=device(r), device_id_type=MESH)
    for r in range(1, NEAR):
        whole(r).wait_recv()

    def combine(n, _):
        cols = tile(n)
        for r in range(NEAR, ne):
            back_copy(r, n).wait_recv()
        zt = jnp.dot(pick[...], zrecv[:, :, cols].reshape(ne * cap, NT), preferred_element_type=jnp.float32)
        y = h_ref[:, cols].astype(jnp.float32) + (meta_ref[:, 2:3] * zt[:t] + meta_ref[:, 3:4] * zt[t:])
        y_ref[:, cols] = y.astype(jnp.bfloat16)

        @pl.when(n > 0)
        def _():
            leave(n - 1).start()
        return 0
    leave = lambda n: pltpu.make_async_copy(y_ref.at[:, tile(n)], yout_ref.at[:, tile(n)], ys.at[0])
    lax.fori_loop(0, nz, combine, 0)
    leave(nz - 1).start()
    for r in range(1, ne):
        out_copy(r).wait_send()
        whole(r).wait_send()
    pltpu.make_async_copy(y_ref, yout_ref, ys.at[0]).wait()


def moe_fast(h, slot, meta, w1g, w1u, w2, cap, cid):
    t, hd = h.shape
    ne = slot.shape[0]
    vm = pl.BlockSpec(memory_space=pltpu.VMEM)
    hb = pl.BlockSpec(memory_space=pl.ANY)
    bf = jnp.bfloat16
    ff = w2.shape[0]
    return pl.pallas_call(
        functools.partial(moe_kernel, ne, cap),
        in_specs=[hb, vm, vm, hb, hb, hb], out_specs=hb,
        out_shape=jax.ShapeDtypeStruct((t, hd), bf),
        scratch_shapes=[pltpu.VMEM((t, hd), bf), pltpu.VMEM((t, hd), bf), pltpu.VMEM((ne, cap, hd), bf), pltpu.VMEM((ne, cap, hd), bf), pltpu.VMEM((NEAR * cap, ff), bf),
                        pltpu.VMEM((ne, cap, hd), bf), pltpu.VMEM((ne, cap, hd), bf), pltpu.VMEM((ne * cap, t), bf), pltpu.VMEM((2 * t, ne * cap), bf),
                        pltpu.VMEM((2, 2, hd, FT), bf), pltpu.VMEM((2, ff, NT), bf)]
                       + [pltpu.SemaphoreType.DMA((ne,))] * 4 + [pltpu.SemaphoreType.DMA((ne - NEAR, hd // NT))] + [pltpu.SemaphoreType.DMA((2, 2)), pltpu.SemaphoreType.DMA((2,)), pltpu.SemaphoreType.DMA((1,)), pltpu.SemaphoreType.DMA((1,))],
        compiler_params=pltpu.CompilerParams(collective_id=cid, has_side_effects=True, vmem_limit_bytes=63 * 1024 * 1024),
        name='moe')(h, slot, meta, w1g, w1u, w2)


def settle_kernel(parts, a_ref, b_ref, buf, ins, outs):
    n = a_ref.shape[0] // parts
    rows = [pl.ds(i * n, n) for i in range(parts)]
    into = [pltpu.make_async_copy(a_ref.at[r], buf.at[r], ins.at[i]) for i, r in enumerate(rows)]
    away = [pltpu.make_async_copy(buf.at[r], b_ref.at[r], outs.at[i]) for i, r in enumerate(rows)]
    for cpy in into:
        cpy.start()
    for i in range(parts):
        into[i].wait()
        away[i].start()
    for cpy in away:
        cpy.wait()


def settle(y, parts=8):
    hb = pl.BlockSpec(memory_space=pl.ANY)
    dma = pltpu.SemaphoreType.DMA((parts,))
    return pl.pallas_call(functools.partial(settle_kernel, parts), in_specs=[hb], out_specs=hb, out_shape=jax.ShapeDtypeStruct(y.shape, y.dtype),
                          scratch_shapes=[pltpu.VMEM(y.shape, y.dtype), dma, dma], name='settle')(y)


D = 128
PIECES = 4
CHUNKS = 4
HOOKS = (2, 8, 13)


def mate(r):
    t = lax.axis_index('tp')
    core = lax.rem(lax.rem(t, 2) + lax.rem(r, 2), 2)
    xx = lax.rem(t // 2 + r // 2, 2)
    return xx * 2 + core


def segment(t, cp):
    c = lax.axis_index('cp')
    return jnp.where(t < 2, c, 2 * cp - 1 - c)


def remote(src, dst, send, recv, dev):
    return pltpu.make_async_remote_copy(src_ref=src, dst_ref=dst, send_sem=send, recv_sem=recv, device_id=dev, device_id_type=MESH)


def route(ne, cp, idx_ref, gate_ref, slot_ref, meta_ref, cnt):
    t = idx_ref.shape[1]
    lab = lax.broadcasted_iota(jnp.int32, (128, t), 0)
    named = [idx_ref[i:i + 1, :] == lab for i in range(2)]
    hit = (named[0] | named[1]).astype(jnp.float32)
    before = (lax.broadcasted_iota(jnp.int32, (t, t), 0) < lax.broadcasted_iota(jnp.int32, (t, t), 1)).astype(jnp.bfloat16)
    rank = jnp.dot(hit.astype(jnp.bfloat16), before, preferred_element_type=jnp.float32)
    slot_ref[...] = jnp.where(hit > 0, rank, -1.0)[:ne].astype(jnp.int32)
    cnt[...] = jnp.broadcast_to(jnp.sum(hit[:8], axis=1, keepdims=True), (8, 128)).astype(jnp.int32)
    me = lax.axis_index('cp') * (ne // cp) + lax.axis_index('tp')
    place = jnp.bitwise_xor(lab, me).astype(jnp.float32) * (2 * t // ne) + rank
    meta = jnp.zeros((128, t), jnp.float32)
    for i in range(2):
        at = jnp.sum(jnp.where(named[i], place, 0.0), axis=0, keepdims=True)
        meta = jnp.where(lab == i, at, jnp.where(lab == 2 + i, gate_ref[i:i + 1, :], meta))
    meta_ref[...] = jnp.transpose(meta)


def front_kernel(cp, ne, x_ref, idx_ref, gate_ref, wq_ref, wk_ref, wv_ref, wo_ref, h_ref, worst_ref, slot_ref, meta_ref,
                 cnt, all_ref, xv, xs, wqb, wkvb, q_ref, kv_ref, wof, ocat, st,
                 cs, cr, as_, ar_, fs, fr, bs, br, ks, kr, ws, xs_, xr_, ys_, yr_, ds_, dr_, os_, or_, ls_, hs_):
    t, hd = x_ref.shape
    c = lax.axis_index('cp')
    loads = [pltpu.make_async_copy(wk_ref, wkvb.at[:, :D], ws.at[0]), pltpu.make_async_copy(wv_ref, wkvb.at[:, D:], ws.at[1]),
             pltpu.make_async_copy(wq_ref, wqb, ws.at[2])]
    hail(range(1, ne))
    loads.append(pltpu.make_async_copy(x_ref, xv, ws.at[3]))
    for ld in reversed(loads):
        ld.start()
    pl.semaphore_wait(pltpu.get_barrier_semaphore(), ne - 1)

    step = t // PIECES
    rows = lambda p: pl.ds(pl.multiple_of(p * step, 16), step)
    across = lambda p: remote(x_ref.at[rows(p)], xs.at[1, rows(p)], as_.at[p], ar_.at[p], device(2))
    onward = lambda p: remote(xs.at[1, rows(p)], xs.at[2, rows(p)], fs.at[p], fr.at[p], device(1))
    beside = remote(x_ref, xs.at[0], bs.at[0], br.at[0], device(1))
    for p in range(2):
        across(p).start()
    beside.start()
    route(ne, cp, idx_ref, gate_ref, slot_ref, meta_ref, cnt)
    all_ref[0] = cnt[...]
    counts = [remote(cnt, all_ref.at[r], cs.at[r], cr.at[r], device(r)) for r in range(1, ne)]

    w = wo_ref.shape[0]
    heads = w // D
    half = w // 2
    cut = half // CHUNKS
    at = lambda base, j: pl.ds(pl.multiple_of(base + j * cut, 16), cut)
    first, second = c * half, (1 - c) * half
    mine = pltpu.make_async_copy(wo_ref, wof.at[:w], ls_.at[0])
    xc = [remote(wo_ref.at[at(first, j)], wof.at[at(2 * w + first, j)], xs_.at[j], xr_.at[j], device(2)) for j in range(CHUNKS)]
    yc = [remote(wof.at[at(2 * w + first, j)], wof.at[at(2 * w + first, j)], ys_.at[j], yr_.at[j], device(4)) for j in range(CHUNKS)]
    dx = [remote(wof.at[at(2 * w + first, j)], wof.at[at(3 * w + first, j)], ds_.at[j], dr_.at[j], device(1)) for j in range(CHUNKS)]
    dy = [remote(wof.at[at(2 * w + second, j)], wof.at[at(3 * w + second, j)], ds_.at[CHUNKS + j], dr_.at[CHUNKS + j], device(1)) for j in range(CHUNKS)]
    whole = remote(wo_ref, wof.at[pl.ds(w, w)], ds_.at[2 * CHUNKS], dr_.at[2 * CHUNKS], device(1))

    def relay_x(j):
        xc[j].wait_recv()
        yc[j].start()
        dx[j].start()

    def relay_y(j):
        yc[j].wait_recv()
        dy[j].start()

    def pair(i, base, n):
        return remote(kv_ref.at[pl.ds(base, n)], kv_ref.at[pl.ds(base, n)], ks.at[i], kr.at[i], device(4))

    def project(block, r, off, n, i):
        tt = mate(r)
        base = pl.multiple_of(segment(tt, cp) * (2 * t) + lax.rem(tt, 2) * t + off, 16)
        kv_ref[pl.ds(base, n), :] = jnp.dot(block, wkvb[...], preferred_element_type=jnp.float32).astype(jnp.bfloat16)
        qb = pl.multiple_of(tt * t + off, 16)
        q_ref[pl.ds(qb, n), :] = jnp.dot(block, wqb[...], preferred_element_type=jnp.float32).astype(jnp.bfloat16)
        pair(i, base, n).start()

    for cc in counts:
        cc.start()
    for p in range(2, PIECES):
        across(p).start()
    for ld in loads:
        ld.wait()
    project(xv[...], 0, 0, t, 0)
    beside.wait_recv()
    project(xs[0], 1, 0, t, 1)

    def land(p, _):
        across(p).wait_recv()
        onward(p).start()

        @pl.when(p == 2)
        def _():
            for cpy in xc:
                cpy.start()
        project(xs[1, rows(p)], 2, p * step, step, 2 + 2 * p)
        onward(p).wait_recv()
        project(xs[2, rows(p)], 3, p * step, step, 3 + 2 * p)
        return 0
    lax.fori_loop(0, PIECES, land, 0)
    mine.start()
    whole.start()
    for cc in counts:
        cc.wait_recv()
    worst_ref[0, 0] = jnp.max(all_ref[...])
    for i in range(2):
        pair(i, 0, t).wait_recv()
    for i in range(2, 2 + 2 * PIECES):
        pair(i, 0, step).wait_recv()
    for p in range(PIECES):
        onward(p).wait_send()

    scale = D ** -0.5 * math.log2(math.e)
    mask = lax.broadcasted_iota(jnp.int32, (t, t), 1) <= lax.broadcasted_iota(jnp.int32, (t, t), 0)
    M, L, A = 0, heads, 2 * heads

    def lanes(p):
        s = p[:, :128]
        for a in range(128, t, 128):
            s = s + p[:, a:a + 128]
        return s

    def which(b):
        return jnp.where(b < 2, b + 2, 3 - b)

    def give(b):
        r = which(b)
        cols = pl.ds(pl.multiple_of(r * w, 128), w)
        return remote(xs.at[2, :, cols], ocat.at[:, cols], os_.at[r], or_.at[r], (lax.axis_index('dp'), c, mate(r)))

    def block(b, u):
        r = which(b)
        tt = mate(r)
        qb = pl.multiple_of(tt * t, t)
        nfull = segment(tt, cp) * 2 + lax.rem(tt, 2)

        def scores(h, j):
            k = kv_ref[pl.ds(pl.multiple_of(j * t, t), t), :D]
            q = q_ref[pl.ds(qb, t), h * D:(h + 1) * D]
            return lax.dot_general(q, k, (((1,), (1,)), ((), ())), preferred_element_type=jnp.float32) * scale

        def pv(p, j):
            v = kv_ref[pl.ds(pl.multiple_of(j * t, t), t), D:]
            return jnp.dot(p.astype(jnp.bfloat16), v, preferred_element_type=jnp.float32)

        for h in range(heads):
            s = jnp.where(mask, scores(h, nfull), -1e30)
            m = jnp.max(s, axis=1, keepdims=True)
            p = jnp.where(mask, jnp.exp2(s - m), 0.0)
            st[M + h] = jnp.broadcast_to(m, (t, 128))
            st[L + h] = lanes(p)
            st[A + h] = pv(p, nfull)

        @pl.when(b > 0)
        def _():
            give(b - 1).start()

        def body(j, _):
            for n, at_unit in enumerate(HOOKS):
                @pl.when(u + j == at_unit)
                def _():
                    relay_x(n)
            for h in range(heads):
                s = scores(h, j)
                mo = st[M + h]
                mn = jnp.maximum(mo, jnp.max(s, axis=1, keepdims=True))
                p = jnp.exp2(s - jnp.concatenate([mn] * (t // 128), axis=1))
                al = jnp.exp2(mo - mn)
                st[M + h] = mn
                st[L + h] = st[L + h] * al + lanes(p)
                st[A + h] = st[A + h] * al + pv(p, j)
            return 0

        lax.fori_loop(0, nfull, body, 0)
        for h in range(heads):
            l = jnp.sum(st[L + h], axis=1, keepdims=True)
            xs[2, :, pl.ds(pl.multiple_of(r * w + h * D, 128), D)] = (st[A + h] / l).astype(jnp.bfloat16)
        return u + nfull

    lax.fori_loop(0, 4, block, 0)
    ocat[:, :w] = xs[2, :, :w]

    tile = lambda n: pl.ds(pl.multiple_of(n * NT, NT), NT)
    per = NT // 128

    def held(n):
        return jnp.concatenate([st[n * per + i] for i in range(per)], axis=1)

    def add(lo, hi, fresh):
        def one(n, _):
            s = jnp.dot(ocat[:, lo * w:hi * w], wof[lo * w:hi * w, tile(n)], preferred_element_type=jnp.float32)
            if not fresh:
                s = s + held(n)
            for i in range(per):
                st[n * per + i] = s[:, i * 128:(i + 1) * 128]
            return 0
        lax.fori_loop(0, hd // NT, one, 0)

    mine.wait()
    whole.wait_recv()
    give(2).wait_recv()
    add(0, 2, True)
    relay_y(0)
    for j in range(len(HOOKS), CHUNKS):
        relay_x(j)
    for j in range(1, CHUNKS):
        relay_y(j)
    for j in range(CHUNKS):
        dx[j].wait_recv()
        dy[j].wait_recv()
    give(0).wait_recv()
    add(2, 3, False)
    give(1).wait_recv()
    out = lambda n: pltpu.make_async_copy(xs.at[0, :, tile(n)], h_ref.at[:, tile(n)], hs_.at[0])

    def last(n, _):
        s = held(n) + jnp.dot(ocat[:, 3 * w:], wof[3 * w:, tile(n)], preferred_element_type=jnp.float32)
        xs[0, :, tile(n)] = (xv[:, tile(n)].astype(jnp.float32) + s).astype(jnp.bfloat16)

        @pl.when(n > 0)
        def _():
            out(n - 1).start()
        return 0
    lax.fori_loop(0, hd // NT, last, 0)
    out(hd // NT - 1).start()
    for p in range(PIECES):
        across(p).wait_send()
    for i in range(2):
        pair(i, 0, t).wait_send()
    for i in range(2, 2 + 2 * PIECES):
        pair(i, 0, step).wait_send()
    for cpy in counts + [beside] + xc + yc + dx + dy + [whole, give(0), give(1), give(2)]:
        cpy.wait_send()
    pltpu.make_async_copy(xs.at[0], h_ref, hs_.at[0]).wait()


def front(x, idx, gates, wq, wk, wv, wo, cp, ne, cid):
    t, hd = x.shape
    tp = ne // cp
    w = wo.shape[0]
    vm = pl.BlockSpec(memory_space=pltpu.VMEM)
    hb = pl.BlockSpec(memory_space=pl.ANY)
    bf = jnp.bfloat16
    dma = lambda n: pltpu.SemaphoreType.DMA((n,))
    nk = 2 + 2 * PIECES
    nd = 2 * CHUNKS + 1
    return pl.pallas_call(
        functools.partial(front_kernel, cp, ne),
        in_specs=[hb, vm, vm, hb, hb, hb, hb], out_specs=[hb, pl.BlockSpec(memory_space=pltpu.SMEM), vm, vm],
        out_shape=[jax.ShapeDtypeStruct((t, hd), bf), jax.ShapeDtypeStruct((1, 1), jnp.int32), jax.ShapeDtypeStruct((ne, t), jnp.int32), jax.ShapeDtypeStruct((t, 128), jnp.float32)],
        scratch_shapes=[pltpu.VMEM((8, 128), jnp.int32), pltpu.VMEM((ne, 8, 128), jnp.int32), pltpu.VMEM((t, hd), bf), pltpu.VMEM((3, t, hd), bf), pltpu.VMEM(wq.shape, bf), pltpu.VMEM((hd, 2 * D), bf),
                        pltpu.VMEM((tp * t, w), bf), pltpu.VMEM((ne * t, 2 * D), bf), pltpu.VMEM((tp * w, hd), bf), pltpu.VMEM((t, tp * w), bf), pltpu.VMEM((hd // 128, t, 128), jnp.float32),
                        dma(ne), dma(ne), dma(PIECES), dma(PIECES), dma(PIECES), dma(PIECES), dma(1), dma(1), dma(nk), dma(nk), dma(4),
                        dma(CHUNKS), dma(CHUNKS), dma(CHUNKS), dma(CHUNKS), dma(nd), dma(nd), dma(4), dma(4), dma(1), dma(1)],
        compiler_params=pltpu.CompilerParams(collective_id=cid, has_side_effects=True, vmem_limit_bytes=67043328),
        name='front')(x, idx.T, gates.T, wq, wk, wv, wo)


def expert_ffn(rows, wg, wu, wd):
    gg = jnp.dot(rows, wg, preferred_element_type=jnp.float32)
    uu = jnp.dot(rows, wu, preferred_element_type=jnp.float32)
    act = (jax.nn.silu(gg) * uu).astype(jnp.bfloat16)
    return jnp.dot(act, wd, preferred_element_type=jnp.float32).astype(jnp.bfloat16)


def moe_any(h, slot, idx, gates, wg, wu, wd):
    t, hd = h.shape
    ne = slot.shape[0]
    cap = 4 * t // ne
    pick = (slot[:, None, :] == jnp.arange(cap)[None, :, None]).astype(jnp.bfloat16).reshape(ne * cap, t)
    send = jnp.dot(pick, h, preferred_element_type=jnp.float32).astype(jnp.bfloat16)
    recv = lax.all_to_all(send.reshape(ne, cap, hd), ('cp', 'tp'), 0, 0, tiled=True)
    z = expert_ffn(recv.reshape(ne * cap, hd), wg, wu, wd)
    back = lax.all_to_all(z.reshape(ne, cap, hd), ('cp', 'tp'), 0, 0, tiled=True).reshape(ne * cap, hd)
    flat = jnp.arange(ne * cap)
    y = h.astype(jnp.float32)
    for k in range(2):
        mine = jnp.sum(jnp.where(idx[:, k][None, :] == jnp.arange(ne)[:, None], jnp.arange(ne)[:, None] * cap + slot, 0), axis=0)
        sel = (mine[:, None] == flat[None, :]).astype(jnp.bfloat16)
        y = y + gates[:, k:k + 1] * jnp.dot(sel, back, preferred_element_type=jnp.float32)
    return y.astype(jnp.bfloat16)


def solution(mesh):
    cp = mesh.shape['cp']
    tp = mesh.shape['tp']
    ne = cp * tp
    rows_spec = P(('dp', 'cp', 'tp'), None)
    exp_spec = P(('cp', 'tp'), None, None)

    def local(x, idx, gates, wq, wk, wv, wo, w1g, w1u, w2):
        t, hd = x.shape
        h, worst, slot, meta = front(x, idx, gates, wq, wk, wv, wo, cp, ne, 1)

        def tight(h):
            return moe_fast(h, slot, meta, w1g[0], w1u[0], w2[0], t // 4, 3)

        def roomy(h):
            return moe_any(h, slot, idx, gates, w1g[0], w1u[0], w2[0])

        return settle(lax.cond(worst[0, 0] <= t // 4, tight, roomy, h))

    return jax.shard_map(local, mesh=mesh, in_specs=(rows_spec, rows_spec, rows_spec, P(None, 'tp'), P(None, 'tp'), P(None, 'tp'), P('tp', None), exp_spec, exp_spec, exp_spec), out_specs=rows_spec, check_vma=False)
```
